8 devices in a mesh: dp: 1 (over z), cols: 2 (over y), rows: 4 (over x, core).
Axes of the slice: x: 2, y: 2, z: 1, core: 2. Of those that a mesh axis runs over, the one named last changes fastest.
Arguments:
- frames: bfloat16 [32, 1, 128, 64, 64], P(None, 'dp', 'rows', 'cols')
- w_in: bfloat16 [3, 3, 64, 768], replicated
- w_rec: bfloat16 [3, 3, 192, 768], replicated
- gate_bias: float32 [768], replicated
- h_init: bfloat16 [1, 128, 64, 192], P('dp', 'rows', 'cols')
- c_init: float32 [1, 128, 64, 192], P('dp', 'rows', 'cols')
Outputs:
- output 1: bfloat16 [32, 1, 128, 64, 192], P(None, 'dp', 'rows', 'cols')
- output 2: float32 [1, 128, 64, 192], P('dp', 'rows', 'cols')
All inputs are finite; a program needn't handle non-finite values.
Results may differ from the reference program's by a relative error of at most 0.00490482.
Values are sent between devices in bfloat16 or wider.
A program may use at most 1 GiB of HBM per device.

```python
import jax
import jax.numpy as jnp
from jax import lax

STEPS = 32
BATCH = 1
GRID_H = 128
GRID_W = 64
C_IN = 64
C_HID = 192

CONV_DIMS = ("NHWC", "HWIO", "NHWC")


def setup_inputs(seed: int = 0, part: int = 0) -> dict:
    part_key = jax.random.fold_in(jax.random.key(seed), part)
    k_frames, k_hid, k_cell = jax.random.split(part_key, 3)
    k_win, k_wrec, k_bias = jax.random.split(jax.random.key(seed + 1), 3)
    frames = jax.random.normal(k_frames, (STEPS, BATCH, GRID_H, GRID_W, C_IN), jnp.float32)
    w_in = jax.random.normal(k_win, (3, 3, C_IN, 4 * C_HID), jnp.float32) * (9 * C_IN) ** -0.5
    w_rec = jax.random.normal(k_wrec, (3, 3, C_HID, 4 * C_HID), jnp.float32) * (2.0 * (9 * C_HID) ** -0.5)
    forget_shift = jnp.concatenate([jnp.zeros((C_HID,), jnp.float32), jnp.ones((C_HID,), jnp.float32), jnp.zeros((2 * C_HID,), jnp.float32)])
    gate_bias = 0.5 * jax.random.normal(k_bias, (4 * C_HID,), jnp.float32) + forget_shift
    h_init = 0.5 * jax.random.normal(k_hid, (BATCH, GRID_H, GRID_W, C_HID), jnp.float32)
    c_init = jax.random.normal(k_cell, (BATCH, GRID_H, GRID_W, C_HID), jnp.float32)
    return {
        "frames": frames.astype(jnp.bfloat16),
        "w_in": w_in.astype(jnp.bfloat16),
        "w_rec": w_rec.astype(jnp.bfloat16),
        "gate_bias": gate_bias,
        "h_init": h_init.astype(jnp.bfloat16),
        "c_init": c_init,
    }


def conv_same(operand, kernel):
    return lax.conv_general_dilated(operand.astype(jnp.float32), kernel, (1, 1), "SAME", dimension_numbers=CONV_DIMS)


def reference(frames, w_in, w_rec, gate_bias, h_init, c_init):
    w_in32 = w_in.astype(jnp.float32)
    w_rec32 = w_rec.astype(jnp.float32)

    def time_step(carry_in, frame_t):
        h_prev, c_prev = carry_in
        gate_pre = conv_same(frame_t, w_in32) + conv_same(h_prev, w_rec32) + gate_bias
        gate_i, gate_f, gate_o, gate_g = jnp.split(gate_pre, 4, axis=-1)
        c_next = jax.nn.sigmoid(gate_f) * c_prev + jax.nn.sigmoid(gate_i) * jnp.tanh(gate_g)
        h_next = (jax.nn.sigmoid(gate_o) * jnp.tanh(c_next)).astype(jnp.bfloat16)
        return (h_next, c_next), h_next

    (h_last, c_last), hidden_seq = lax.scan(time_step, (h_init, c_init), frames)
    return hidden_seq, c_last
```

```python
import functools

import jax
import jax.numpy as jnp
from jax import lax
from jax.experimental import pallas as pl
from jax.experimental.pallas import tpu as pltpu
from jax.sharding import PartitionSpec as P

MESH = pl.DeviceIdType.MESH
BF16, F32 = jnp.bfloat16, jnp.float32
PAD = 8
HALO_L, COL_0, COL_1, COL_30, COL_31, HALO_R = range(6)
UP, DOWN, LEFT, RIGHT = range(4)
UL, UR, DL, DR = range(4)


def half_tanh(x):
    return 0.5 * jnp.tanh(0.5 * x) + 0.5


def kernel(n_rows, n_cols, steps, th, tw,
           frames, w, bias, h_init, c_init, hs, c_out,
           s0, s1, s2, xm, xt, fx, em, et, cm, ct, colm, colt,
           ga, gb, gc, gd, gr, fr, ho, send, land, corner,
           send_sem, recv_sem, fr_sem, out_sem):
    row, col = lax.axis_index("rows"), lax.axis_index("cols")
    has = {UP: row > 0, DOWN: row < n_rows - 1, LEFT: col > 0, RIGHT: col < n_cols - 1}
    shifts = (s0, s1, s2)
    cells = th * tw

    def routes(slot):
        half = tw // 2
        edge = lambda place: land.at[slot, place]
        point = lambda place: corner.at[slot, place]
        return [
            (has[UP], -1, 0, send.at[UP], 0, edge(DOWN)),
            (has[DOWN], 1, 0, send.at[DOWN], 1, edge(UP)),
            (has[LEFT], 0, -1, send.at[LEFT], 2, edge(RIGHT)),
            (has[RIGHT], 0, 1, send.at[RIGHT], 3, edge(LEFT)),
            (has[UP] & has[LEFT], -1, -1, send.at[UP, pl.ds(0, half)], 4, point(DR)),
            (has[UP] & has[RIGHT], -1, 1, send.at[UP, pl.ds(half, half)], 5, point(DL)),
            (has[DOWN] & has[LEFT], 1, -1, send.at[DOWN, pl.ds(0, half)], 6, point(UR)),
            (has[DOWN] & has[RIGHT], 1, 1, send.at[DOWN, pl.ds(half, half)], 7, point(UL)),
        ]

    def copy_of(route, slot):
        _, d_row, d_col, src, index, dst = route
        return pltpu.make_async_remote_copy(
            src_ref=src, dst_ref=dst, send_sem=send_sem.at[index], recv_sem=recv_sem.at[slot, index],
            device_id={"rows": row + d_row, "cols": col + d_col}, device_id_type=MESH)

    def start_sends(slot):
        for route in routes(slot):
            @pl.when(route[0])
            def _():
                copy_of(route, slot).start()

    def wait_sends(slot):
        for route in routes(slot):
            @pl.when(route[0])
            def _():
                copy_of(route, slot).wait_send()

    def wait_recvs(slot):
        came = [has[DOWN], has[UP], has[RIGHT], has[LEFT], has[DOWN] & has[RIGHT], has[DOWN] & has[LEFT],
                has[UP] & has[RIGHT], has[UP] & has[LEFT]]
        for route, condition in zip(routes(slot), came):
            @pl.when(condition)
            def _():
                copy_of(route, slot).wait_recv()

    def frame_copy(t):
        return pltpu.make_async_copy(frames.at[jnp.minimum(t, steps - 1)], fr.at[lax.rem(t, 2)], fr_sem.at[lax.rem(t, 2)])

    def out_copy(t):
        return pltpu.make_async_copy(ho.at[lax.rem(t, 2)], hs.at[t], out_sem.at[lax.rem(t, 2)])

    lane = lax.broadcasted_iota(jnp.int32, (tw, 128), 1)
    low = lane < 64
    scale = jnp.where(low, 1.0, 0.5)
    shift = jnp.where(low, 0.0, 0.5)

    def cell(gates, c_main, c_tail, frame):
        pre = [gates(k) + bias[:, 128 * k:128 * (k + 1)] for k in range(6)]
        n_main = half_tanh(pre[1]) * c_main + half_tanh(pre[0]) * jnp.tanh(pre[3])
        h_main = half_tanh(pre[2]) * jnp.tanh(n_main)
        fore = half_tanh(pre[4])
        back = jnp.tanh(pre[5] * scale) * scale + shift
        n_tail = fore * c_tail + pltpu.roll(fore * back, 64, 1)
        h_tail = back * jnp.tanh(n_tail)
        return n_main, n_tail, h_main, jnp.where(low, frame, h_tail)

    def update_rows(g_ref, g_row, i):
        at = pl.ds(i * tw, tw)
        n_main, n_tail, x_main, x_tail = cell(
            lambda k: g_ref[pl.ds(g_row, tw), 128 * k:128 * (k + 1)], cm[at, :], ct[at, :], fx[at, :])
        cm[at, :] = n_main
        ct[at, :] = n_tail
        xm[pl.ds(PAD + i * tw, tw), :] = x_main
        xt[pl.ds(PAD + i * tw, tw), :] = x_tail

    def form_row(i, slot):
        for part, x in enumerate((xm, xt)):
            for dx in range(3):
                value = x[pl.ds(PAD + i * tw + dx - 1, tw), :].astype(BF16)
                shifts[dx][pl.ds((i + 1) * tw, tw), 128 * part:128 * (part + 1)] = value
        if slot is not None:
            ho[slot, pl.ds(i * tw, tw), 0:128] = xm[pl.ds(PAD + i * tw, tw), :].astype(BF16)
            tail = pltpu.roll(xt[pl.ds(PAD + i * tw, tw), :], 64, 1)
            ho[slot, pl.ds(i * tw, tw), 128:192] = tail[:, :64].astype(BF16)

    def convert_frame(t):
        for i in range(th):
            at = pl.ds(i * tw, tw)
            fx[at, 0:64] = fr[lax.rem(t, 2), at, :].astype(F32)

    def column(x, j, start=0, size=th):
        return x[pl.ds(PAD + start * tw + j, size, stride=tw), :]

    def matmul(g_ref, i, n):
        lhs = [shifts[dx][(i + dy) * tw:(i + dy + n) * tw, :] for dy in range(3) for dx in range(3)]
        g_ref[...] = jnp.dot(jnp.concatenate(lhs, axis=1), w[...], preferred_element_type=F32)

    def ring_matmul():
        lhs = []
        for dy in range(3):
            for dx in range(3):
                pieces = [shifts[dx][dy * tw:(dy + 1) * tw, :], shifts[dx][(th - 1 + dy) * tw:(th + dy) * tw, :]]
                for k in ((HALO_L, COL_0, COL_1)[dx], (COL_30, COL_31, HALO_R)[dx]):
                    at = pl.ds(PAD - 1 + dy, th)
                    pieces.append(jnp.concatenate([em[k, at, :].astype(BF16), et[k, at, :].astype(BF16)], axis=1))
                lhs.append(jnp.concatenate(pieces, axis=0))
        gr[...] = jnp.dot(jnp.concatenate(lhs, axis=1), w[...], preferred_element_type=F32)

    def place_halo(slot):
        for place, r, e_row in ((UP, 0, PAD - 1), (DOWN, th + 1, PAD + th)):
            for part, e in enumerate((em, et)):
                x = (xm, xt)[part]
                lanes = slice(128 * part, 128 * (part + 1))
                value = land[slot, place, :, lanes].astype(F32)
                s1[r * tw:(r + 1) * tw, lanes] = value.astype(BF16)
                s0[r * tw:(r + 1) * tw, lanes] = pltpu.roll(value, 1, 0).astype(BF16)
                s2[r * tw:(r + 1) * tw, lanes] = pltpu.roll(value, tw - 1, 0).astype(BF16)
                for k, j in ((COL_0, 0), (COL_1, 1), (COL_30, tw - 2), (COL_31, tw - 1)):
                    e[k, e_row:e_row + 1, :] = value[j:j + 1, :]
        for part, e in enumerate((em, et)):
            lanes = slice(128 * part, 128 * (part + 1))
            for k, place in ((HALO_L, LEFT), (HALO_R, RIGHT)):
                e[k, PAD:PAD + th, :] = land[slot, place, :, lanes].astype(F32)
            for k, e_row, place, j in ((HALO_L, PAD - 1, UL, 15), (HALO_R, PAD - 1, UR, 0),
                                       (HALO_L, PAD + th, DL, 15), (HALO_R, PAD + th, DR, 0)):
                value = corner[slot, place, :, lanes].astype(F32)
                e[k, e_row:e_row + 1, :] = value[j:j + 1, :]

    def update_ring():
        update_rows(gr, 0, 0)
        update_rows(gr, tw, th - 1)
        for index, (k, j, g_row, place) in enumerate(((COL_0, 0, 2 * tw, LEFT), (COL_31, tw - 1, 2 * tw + th, RIGHT))):
            at = pl.ds(index * th, th)
            n_main, n_tail, x_main, x_tail = cell(
                lambda p: gr[pl.ds(g_row, th), 128 * p:128 * (p + 1)], colm[at, :], colt[at, :],
                fx[pl.ds(j, th, stride=tw), :])
            colm[at, :] = n_main
            colt[at, :] = n_tail
            for part, (x, e, value) in enumerate(((xm, em, x_main), (xt, et, x_tail))):
                e[k, PAD:PAD + th, :] = value
                x[pl.ds(PAD + j, th, stride=tw), :] = value
                send[place, :, 128 * part:128 * (part + 1)] = value.astype(BF16)
        fill_row_sends()

    def fill_row_sends():
        for place, i in ((UP, 0), (DOWN, th - 1)):
            for part, x in enumerate((xm, xt)):
                send[place, :, 128 * part:128 * (part + 1)] = x[pl.ds(PAD + i * tw, tw), :].astype(BF16)

    def finish_last(slot):
        for i in range(25, 31):
            update_rows(gd, (i - 25) * tw, i)
        for k, j in ((COL_0, 0), (COL_31, tw - 1)):
            for x, e in ((xm, em), (xt, et)):
                x[pl.ds(PAD + 24 * tw + j, 8, stride=tw), :] = e[k, PAD + 24:PAD + 32, :]
        for i in range(24, 32):
            form_row(i, slot)
        for k, j in ((COL_1, 1), (COL_30, tw - 2)):
            em[k, PAD:PAD + th, :] = column(xm, j)
            et[k, PAD:PAD + th, :] = column(xt, j)

    def first_blocks():
        matmul(ga, 1, 8)
        matmul(gb, 9, 8)
        for i in range(1, 9):
            update_rows(ga, (i - 1) * tw, i)
        matmul(gc, 17, 8)
        for i in range(9, 17):
            update_rows(gb, (i - 9) * tw, i)

    def late_blocks(slot):
        ring_matmul()
        for i in range(17, 25):
            update_rows(gc, (i - 17) * tw, i)
        matmul(gd, 25, 6)
        update_ring()
        for i in range(24):
            form_row(i, slot)

    frame_copy(0).start()
    frame_copy(1).start()
    land[...] = jnp.zeros_like(land)
    corner[...] = jnp.zeros_like(corner)
    for ref in (em, et):
        ref[...] = jnp.zeros_like(ref)
    for ref in (xm, xt):
        ref[0:PAD, :] = jnp.zeros((PAD, 128), F32)
        ref[PAD + cells:, :] = jnp.zeros((PAD, 128), F32)
    fx[...] = jnp.zeros_like(fx)

    barrier = pltpu.get_barrier_semaphore()
    neighbours = 0
    for condition, d_row, d_col, *_ in routes(0):
        neighbours = neighbours + condition.astype(jnp.int32)

        @pl.when(condition)
        def _():
            pl.semaphore_signal(barrier, inc=1, device_id={"rows": row + d_row, "cols": col + d_col}, device_id_type=MESH)
    pl.semaphore_wait(barrier, neighbours)

    frame_copy(0).wait()

    @pl.loop(0, th)
    def _(i):
        at = pl.ds(pl.multiple_of(i * tw, tw), tw)
        to = pl.ds(pl.multiple_of(PAD + i * tw, 8), tw)
        fx[at, 0:64] = fr[0, at, :].astype(F32)
        xm[to, :] = h_init[at, 0:128].astype(F32)
        tail = h_init[at, 128:192].astype(F32)
        xt[to, :] = jnp.concatenate([fx[at, 0:64], tail], axis=1)
        cm[at, :] = c_init[at, 0:128]
        tail = c_init[at, 128:192]
        ct[at, :] = jnp.concatenate([tail, tail], axis=1)

    for index, (k, j, place) in enumerate(((COL_0, 0, LEFT), (COL_31, tw - 1, RIGHT))):
        at = pl.ds(index * th, th)
        colm[at, :] = cm[pl.ds(j, th, stride=tw), :]
        colt[at, :] = ct[pl.ds(j, th, stride=tw), :]
        for part, (x, e) in enumerate(((xm, em), (xt, et))):
            value = column(x, j)
            e[k, PAD:PAD + th, :] = value
            send[place, :, 128 * part:128 * (part + 1)] = value.astype(BF16)
    for k, j in ((COL_1, 1), (COL_30, tw - 2)):
        em[k, PAD:PAD + th, :] = column(xm, j)
        et[k, PAD:PAD + th, :] = column(xt, j)
    fill_row_sends()
    start_sends(0)
    frame_copy(1).wait()
    frame_copy(2).start()
    for i in range(th):
        form_row(i, None)
    convert_frame(1)
    first_blocks()

    def arrive(t):
        slot = lax.rem(t, 2)
        wait_recvs(slot)
        wait_sends(slot)
        place_halo(slot)

    def body(t, carry):
        slot = lax.rem(t, 2)
        frame_copy(t + 2).wait()
        frame_copy(t + 3).start()

        @pl.when(t >= 2)
        def _():
            out_copy(t - 2).wait()

        @pl.when(t >= 1)
        def _():
            out_copy(t - 1).start()
        arrive(t)
        late_blocks(slot)
        start_sends(1 - slot)
        finish_last(slot)
        convert_frame(t + 2)
        first_blocks()
        return carry

    lax.fori_loop(0, steps - 1, body, 0)

    last = steps - 1
    frame_copy(last + 2).wait()
    out_copy(last - 2).wait()
    out_copy(last - 1).start()
    arrive(last)
    late_blocks(last % 2)
    finish_last(last % 2)
    out_copy(last).start()
    for index, j in enumerate((0, tw - 1)):
        at = pl.ds(index * th, th)
        cm[pl.ds(j, th, stride=tw), :] = colm[at, :]
        ct[pl.ds(j, th, stride=tw), :] = colt[at, :]

    @pl.loop(0, th)
    def _(i):
        at = pl.ds(pl.multiple_of(i * tw, tw), tw)
        c_out[at, 0:128] = cm[at, :]
        c_out[at, 128:192] = pltpu.roll(ct[at, :], 64, 1)[:, :64]
    out_copy(last - 1).wait()
    out_copy(last).wait()


def lane_order(x, c):
    i, f, o, g = (x[..., k * c:(k + 1) * c] for k in range(4))
    return jnp.concatenate([i[..., :128], f[..., :128], o[..., :128], g[..., :128],
                            i[..., 128:], f[..., 128:], g[..., 128:], o[..., 128:]], axis=-1)


def solution(mesh):
    n_rows, n_cols = mesh.shape["rows"], mesh.shape["cols"]
    seq_spec = P(None, "dp", "rows", "cols", None)
    state_spec = P("dp", "rows", "cols", None)

    def local_run(frames, w_in, w_rec, gate_bias, h_init, c_init):
        steps, _, th, tw, c_in = frames.shape
        c_hid = h_init.shape[-1]
        cells = th * tw
        w = jnp.concatenate([w_rec[:, :, :128], w_in, w_rec[:, :, 128:]], axis=2)
        w = lane_order(w.reshape(9 * (c_in + c_hid), 4 * c_hid), c_hid)
        bias = lane_order(gate_bias.reshape(1, 4 * c_hid), c_hid)
        vmem = pl.BlockSpec(memory_space=pltpu.VMEM)
        hbm = pl.BlockSpec(memory_space=pl.ANY)
        run = pl.pallas_call(
            functools.partial(kernel, n_rows, n_cols, steps, th, tw),
            out_shape=(jax.ShapeDtypeStruct((steps, cells, c_hid), BF16), jax.ShapeDtypeStruct((cells, c_hid), F32)),
            in_specs=[hbm, vmem, vmem, vmem, vmem],
            out_specs=(hbm, vmem),
            scratch_shapes=[
                *[pltpu.VMEM(((th + 2) * tw, 256), BF16)] * 3,
                *[pltpu.VMEM((cells + 2 * PAD, 128), F32)] * 2,
                pltpu.VMEM((cells, 128), F32),
                *[pltpu.VMEM((6, th + 2 * PAD, 128), F32)] * 2,
                *[pltpu.VMEM((cells, 128), F32)] * 2,
                *[pltpu.VMEM((2 * th, 128), F32)] * 2,
                *[pltpu.VMEM((8 * tw, 768), F32)] * 3,
                pltpu.VMEM((6 * tw, 768), F32),
                pltpu.VMEM((4 * tw, 768), F32),
                pltpu.VMEM((2, cells, c_in), BF16),
                pltpu.VMEM((2, cells, c_hid), BF16),
                pltpu.VMEM((4, tw, 256), BF16),
                pltpu.VMEM((2, 4, tw, 256), BF16),
                pltpu.VMEM((2, 4, tw // 2, 256), BF16),
                pltpu.SemaphoreType.DMA((8,)),
                pltpu.SemaphoreType.DMA((2, 8)),
                pltpu.SemaphoreType.DMA((2,)),
                pltpu.SemaphoreType.DMA((2,)),
            ],
            compiler_params=pltpu.CompilerParams(collective_id=0, has_side_effects=True, vmem_limit_bytes=60 << 20),
        )
        hidden, c_last = run(frames.reshape(steps, cells, c_in), w, bias,
                             h_init.reshape(cells, c_hid), c_init.reshape(cells, c_hid))
        return hidden.reshape(steps, 1, th, tw, c_hid), c_last.reshape(1, th, tw, c_hid)

    return jax.shard_map(local_run, mesh=mesh, in_specs=(seq_spec, P(), P(), P(), state_spec, state_spec),
                         out_specs=(seq_spec, state_spec), check_vma=False)
```

```python
import functools

import jax
import jax.numpy as jnp
from jax import lax
from jax.experimental import pallas as pl
from jax.experimental.pallas import tpu as pltpu
from jax.sharding import PartitionSpec as P

MESH = pl.DeviceIdType.MESH
BF16, F32 = jnp.bfloat16, jnp.float32
PAD = 8
HALO_L, COL_0, COL_1, COL_30, COL_31, HALO_R = range(6)
UP, DOWN, LEFT, RIGHT = range(4)
UL, UR, DL, DR = range(4)
BLOCK_A, BLOCK_B, BLOCK_C, BLOCK_D = (1, 9), (10, 9), (19, 8), (27, 4)


def half_tanh(x):
    return 0.5 * jnp.tanh(0.5 * x) + 0.5


def kernel(n_rows, n_cols, steps, th, tw,
           frames, w_in, w_rec, gate_bias, h_hbm, c_hbm, hs, c_out,
           s0, s1, s2, xm, xt, fx, em, et, cm, ct, colm, colt,
           ga, gb, gc, gd, gr, wraw, ws, hb, cb, fr, send, land, corner,
           send_sem, recv_sem, fr_sem, in_sem):
    row, col = lax.axis_index("rows"), lax.axis_index("cols")
    has = {UP: row > 0, DOWN: row < n_rows - 1, LEFT: col > 0, RIGHT: col < n_cols - 1}
    shifts = (s0, s1, s2)
    cells = th * tw

    def routes(slot):
        half = tw // 2
        edge = lambda place: land.at[slot, place]
        point = lambda place: corner.at[slot, place]
        return [
            (has[UP], -1, 0, send.at[UP], 0, edge(DOWN)),
            (has[DOWN], 1, 0, send.at[DOWN], 1, edge(UP)),
            (has[LEFT], 0, -1, send.at[LEFT], 2, edge(RIGHT)),
            (has[RIGHT], 0, 1, send.at[RIGHT], 3, edge(LEFT)),
            (has[UP] & has[LEFT], -1, -1, send.at[UP, pl.ds(0, half)], 4, point(DR)),
            (has[UP] & has[RIGHT], -1, 1, send.at[UP, pl.ds(half, half)], 5, point(DL)),
            (has[DOWN] & has[LEFT], 1, -1, send.at[DOWN, pl.ds(0, half)], 6, point(UR)),
            (has[DOWN] & has[RIGHT], 1, 1, send.at[DOWN, pl.ds(half, half)], 7, point(UL)),
        ]

    def copy_of(route, slot):
        _, d_row, d_col, src, index, dst = route
        return pltpu.make_async_remote_copy(
            src_ref=src, dst_ref=dst, send_sem=send_sem.at[index], recv_sem=recv_sem.at[slot, index],
            device_id={"rows": row + d_row, "cols": col + d_col}, device_id_type=MESH)

    def start_sends(slot):
        for route in routes(slot):
            @pl.when(route[0])
            def _():
                copy_of(route, slot).start()

    def wait_sends(slot):
        for route in routes(slot):
            @pl.when(route[0])
            def _():
                copy_of(route, slot).wait_send()

    def wait_recvs(slot):
        came = [has[DOWN], has[UP], has[RIGHT], has[LEFT], has[DOWN] & has[RIGHT], has[DOWN] & has[LEFT],
                has[UP] & has[RIGHT], has[UP] & has[LEFT]]
        for route, condition in zip(routes(slot), came):
            @pl.when(condition)
            def _():
                copy_of(route, slot).wait_recv()

    def frame_copy(t):
        return pltpu.make_async_copy(frames.at[jnp.minimum(t, steps - 1)], fr.at[lax.rem(t, 2)], fr_sem.at[lax.rem(t, 2)])

    weight_copies = [
        pltpu.make_async_copy(w_rec.at[:, pl.ds(0, 128)], wraw.at[:, pl.ds(0, 128)], in_sem.at[0]),
        pltpu.make_async_copy(w_in, wraw.at[:, pl.ds(128, 64)], in_sem.at[1]),
        pltpu.make_async_copy(w_rec.at[:, pl.ds(128, 64)], wraw.at[:, pl.ds(192, 64)], in_sem.at[2]),
    ]
    state_copies = [pltpu.make_async_copy(h_hbm, hb, in_sem.at[3]), pltpu.make_async_copy(c_hbm, cb, in_sem.at[4])]

    bias = lane_order(gate_bias[...], 192)
    lane = lax.broadcasted_iota(jnp.int32, (tw, 128), 1)
    low = lane < 64
    scale = jnp.where(low, 1.0, 0.5)
    shift = jnp.where(low, 0.0, 0.5)

    def cell(gates, c_main, c_tail, frame):
        pre = [gates(k) + bias[:, 128 * k:128 * (k + 1)] for k in range(6)]
        n_main = half_tanh(pre[1]) * c_main + half_tanh(pre[0]) * jnp.tanh(pre[3])
        h_main = half_tanh(pre[2]) * jnp.tanh(n_main)
        fore = half_tanh(pre[4])
        back = jnp.tanh(pre[5] * scale) * scale + shift
        n_tail = fore * c_tail + pltpu.roll(fore * back, 64, 1)
        h_tail = back * jnp.tanh(n_tail)
        return n_main, n_tail, h_main, jnp.where(low, frame, h_tail)

    def update_rows(g_ref, g_row, i):
        at = pl.ds(i * tw, tw)
        n_main, n_tail, x_main, x_tail = cell(
            lambda k: g_ref[pl.ds(g_row, tw), 128 * k:128 * (k + 1)], cm[at, :], ct[at, :], fx[at, :])
        cm[at, :] = n_main
        ct[at, :] = n_tail
        xm[pl.ds(PAD + i * tw, tw), :] = x_main
        xt[pl.ds(PAD + i * tw, tw), :] = x_tail

    def form_row(i, t):
        for part, x in enumerate((xm, xt)):
            for dx in range(3):
                value = x[pl.ds(PAD + i * tw + dx - 1, tw), :].astype(BF16)
                shifts[dx][pl.ds((i + 1) * tw, tw), 128 * part:128 * (part + 1)] = value
        if t is not None:
            hs[t, pl.ds(i * tw, tw), 0:128] = xm[pl.ds(PAD + i * tw, tw), :].astype(BF16)
            tail = pltpu.roll(xt[pl.ds(PAD + i * tw, tw), :], 64, 1)
            hs[t, pl.ds(i * tw, tw), 128:192] = tail[:, :64].astype(BF16)

    def convert_frame(t):
        for i in range(th):
            at = pl.ds(i * tw, tw)
            fx[at, 0:64] = fr[lax.rem(t, 2), at, :].astype(F32)

    def column(x, j, start=0, size=th):
        return x[pl.ds(PAD + start * tw + j, size, stride=tw), :]

    def matmul(g_ref, block):
        i, n = block
        lhs = [shifts[dx][(i + dy) * tw:(i + dy + n) * tw, :] for dy in range(3) for dx in range(3)]
        g_ref[...] = jnp.dot(jnp.concatenate(lhs, axis=1), ws[...], preferred_element_type=F32)

    def ring_matmul():
        lhs = []
        for dy in range(3):
            for dx in range(3):
                pieces = [shifts[dx][dy * tw:(dy + 1) * tw, :], shifts[dx][(th - 1 + dy) * tw:(th + dy) * tw, :]]
                for k in ((HALO_L, COL_0, COL_1)[dx], (COL_30, COL_31, HALO_R)[dx]):
                    at = pl.ds(PAD - 1 + dy, th)
                    pieces.append(jnp.concatenate([em[k, at, :].astype(BF16), et[k, at, :].astype(BF16)], axis=1))
                lhs.append(jnp.concatenate(pieces, axis=0))
        gr[...] = jnp.dot(jnp.concatenate(lhs, axis=1), ws[...], preferred_element_type=F32)

    def place_halo(slot):
        for place, r, e_row in ((UP, 0, PAD - 1), (DOWN, th + 1, PAD + th)):
            for part, e in enumerate((em, et)):
                x = (xm, xt)[part]
                lanes = slice(128 * part, 128 * (part + 1))
                value = land[slot, place, :, lanes].astype(F32)
                s1[r * tw:(r + 1) * tw, lanes] = value.astype(BF16)
                s0[r * tw:(r + 1) * tw, lanes] = pltpu.roll(value, 1, 0).astype(BF16)
                s2[r * tw:(r + 1) * tw, lanes] = pltpu.roll(value, tw - 1, 0).astype(BF16)
                for k, j in ((COL_0, 0), (COL_1, 1), (COL_30, tw - 2), (COL_31, tw - 1)):
                    e[k, e_row:e_row + 1, :] = value[j:j + 1, :]
        for part, e in enumerate((em, et)):
            lanes = slice(128 * part, 128 * (part + 1))
            for k, place in ((HALO_L, LEFT), (HALO_R, RIGHT)):
                e[k, PAD:PAD + th, :] = land[slot, place, :, lanes].astype(F32)
            for k, e_row, place, j in ((HALO_L, PAD - 1, UL, 15), (HALO_R, PAD - 1, UR, 0),
                                       (HALO_L, PAD + th, DL, 15), (HALO_R, PAD + th, DR, 0)):
                value = corner[slot, place, :, lanes].astype(F32)
                e[k, e_row:e_row + 1, :] = value[j:j + 1, :]

    def update_ring():
        update_rows(gr, 0, 0)
        update_rows(gr, tw, th - 1)
        for index, (k, j, g_row, place) in enumerate(((COL_0, 0, 2 * tw, LEFT), (COL_31, tw - 1, 2 * tw + th, RIGHT))):
            at = pl.ds(index * th, th)
            n_main, n_tail, x_main, x_tail = cell(
                lambda p: gr[pl.ds(g_row, th), 128 * p:128 * (p + 1)], colm[at, :], colt[at, :],
                fx[pl.ds(j, th, stride=tw), :])
            colm[at, :] = n_main
            colt[at, :] = n_tail
            for part, (x, e, value) in enumerate(((xm, em, x_main), (xt, et, x_tail))):
                e[k, PAD:PAD + th, :] = value
                x[pl.ds(PAD + j, th, stride=tw), :] = value
                send[place, :, 128 * part:128 * (part + 1)] = value.astype(BF16)
        fill_row_sends()

    def fill_row_sends():
        for place, i in ((UP, 0), (DOWN, th - 1)):
            for part, x in enumerate((xm, xt)):
                send[place, :, 128 * part:128 * (part + 1)] = x[pl.ds(PAD + i * tw, tw), :].astype(BF16)

    def update_block(g_ref, block):
        for i in range(block[0], sum(block)):
            update_rows(g_ref, (i - block[0]) * tw, i)

    def finish_last():
        update_block(gd, BLOCK_D)
        first = th - 8
        for k, j in ((COL_0, 0), (COL_31, tw - 1)):
            for x, e in ((xm, em), (xt, et)):
                x[pl.ds(PAD + first * tw + j, 8, stride=tw), :] = e[k, PAD + first:PAD + th, :]
        for k, j in ((COL_1, 1), (COL_30, tw - 2)):
            em[k, PAD:PAD + th, :] = column(xm, j)
            et[k, PAD:PAD + th, :] = column(xt, j)

    def first_blocks(t, next_frame):
        matmul(ga, BLOCK_A)
        for i in range(sum(BLOCK_A) + 1, sum(BLOCK_B) + 1):
            form_row(i, t)
        if t is not None:
            finish_last()
        for i in range(sum(BLOCK_B) + 1, th):
            form_row(i, t)
        convert_frame(next_frame)
        matmul(gb, BLOCK_B)
        update_block(ga, BLOCK_A)
        matmul(gc, BLOCK_C)
        update_block(gb, BLOCK_B)

    def late_blocks(t):
        ring_matmul()
        update_block(gc, BLOCK_C)
        matmul(gd, BLOCK_D)
        update_ring()
        for i in range(sum(BLOCK_A) + 1):
            form_row(i, t)

    for copy in state_copies:
        copy.start()
    frame_copy(0).start()
    for copy in weight_copies:
        copy.start()
    frame_copy(1).start()
    land[...] = jnp.zeros_like(land)
    corner[...] = jnp.zeros_like(corner)
    for ref in (em, et):
        ref[...] = jnp.zeros_like(ref)
    for ref in (xm, xt):
        ref[0:PAD, :] = jnp.zeros((PAD, 128), F32)
        ref[PAD + cells:, :] = jnp.zeros((PAD, 128), F32)
    fx[...] = jnp.zeros_like(fx)

    barrier = pltpu.get_barrier_semaphore()
    neighbours = 0
    for condition, d_row, d_col, *_ in routes(0):
        neighbours = neighbours + condition.astype(jnp.int32)

        @pl.when(condition)
        def _():
            pl.semaphore_signal(barrier, inc=1, device_id={"rows": row + d_row, "cols": col + d_col}, device_id_type=MESH)
    pl.semaphore_wait(barrier, neighbours)

    frame_copy(0).wait()
    for copy in state_copies:
        copy.wait()

    @pl.loop(0, th)
    def _(i):
        at = pl.ds(pl.multiple_of(i * tw, tw), tw)
        to = pl.ds(pl.multiple_of(PAD + i * tw, 8), tw)
        fx[at, 0:64] = fr[0, at, :].astype(F32)
        xm[to, :] = hb[at, 0:128].astype(F32)
        tail = hb[at, 128:192].astype(F32)
        xt[to, :] = jnp.concatenate([fx[at, 0:64], tail], axis=1)
        cm[at, :] = cb[at, 0:128]
        tail = cb[at, 128:192]
        ct[at, :] = jnp.concatenate([tail, tail], axis=1)

    for index, (k, j, place) in enumerate(((COL_0, 0, LEFT), (COL_31, tw - 1, RIGHT))):
        at = pl.ds(index * th, th)
        colm[at, :] = cm[pl.ds(j, th, stride=tw), :]
        colt[at, :] = ct[pl.ds(j, th, stride=tw), :]
        for part, (x, e) in enumerate(((xm, em), (xt, et))):
            value = column(x, j)
            e[k, PAD:PAD + th, :] = value
            send[place, :, 128 * part:128 * (part + 1)] = value.astype(BF16)
    for k, j in ((COL_1, 1), (COL_30, tw - 2)):
        em[k, PAD:PAD + th, :] = column(xm, j)
        et[k, PAD:PAD + th, :] = column(xt, j)
    fill_row_sends()
    start_sends(0)
    frame_copy(1).wait()
    frame_copy(2).start()
    for i in range(sum(BLOCK_A) + 1):
        form_row(i, None)
    for copy in weight_copies:
        copy.wait()

    @pl.loop(0, 9)
    def _(tap):
        for k in range(0, 256, 64):
            at = pl.ds(pl.multiple_of(tap * 256 + k, 64), 64)
            ws[at, :] = lane_order(wraw[tap, k:k + 64, :], 192)
    first_blocks(None, 1)

    def arrive(t):
        slot = lax.rem(t, 2)
        wait_recvs(slot)
        wait_sends(slot)
        place_halo(slot)

    def body(t, carry):
        slot = lax.rem(t, 2)
        frame_copy(t + 2).wait()
        frame_copy(t + 3).start()
        arrive(t)
        late_blocks(t)
        start_sends(1 - slot)
        first_blocks(t, t + 2)
        return carry

    lax.fori_loop(0, steps - 1, body, 0)

    last = steps - 1
    frame_copy(last + 2).wait()
    arrive(last)
    late_blocks(last)
    finish_last()
    for i in range(sum(BLOCK_A) + 1, th):
        form_row(i, last)
    for index, j in enumerate((0, tw - 1)):
        at = pl.ds(index * th, th)
        cm[pl.ds(j, th, stride=tw), :] = colm[at, :]
        ct[pl.ds(j, th, stride=tw), :] = colt[at, :]

    @pl.loop(0, th)
    def _(i):
        at = pl.ds(pl.multiple_of(i * tw, tw), tw)
        c_out[at, 0:128] = cm[at, :]
        c_out[at, 128:192] = pltpu.roll(ct[at, :], 64, 1)[:, :64]


def lane_order(x, c):
    i, f, o, g = (x[..., k * c:(k + 1) * c] for k in range(4))
    return jnp.concatenate([i[..., :128], f[..., :128], o[..., :128], g[..., :128],
                            i[..., 128:], f[..., 128:], g[..., 128:], o[..., 128:]], axis=-1)


def solution(mesh):
    n_rows, n_cols = mesh.shape["rows"], mesh.shape["cols"]
    seq_spec = P(None, "dp", "rows", "cols", None)
    state_spec = P("dp", "rows", "cols", None)

    def local_run(frames, w_in, w_rec, gate_bias, h_init, c_init):
        steps, _, th, tw, c_in = frames.shape
        c_hid = h_init.shape[-1]
        cells = th * tw
        vmem = pl.BlockSpec(memory_space=pltpu.VMEM)
        hbm = pl.BlockSpec(memory_space=pl.ANY)
        run = pl.pallas_call(
            functools.partial(kernel, n_rows, n_cols, steps, th, tw),
            out_shape=(pltpu.VMEM((steps, cells, c_hid), BF16), jax.ShapeDtypeStruct((cells, c_hid), F32)),
            in_specs=[hbm, hbm, hbm, vmem, hbm, hbm],
            out_specs=(vmem, vmem),
            scratch_shapes=[
                *[pltpu.VMEM(((th + 2) * tw, 256), BF16)] * 3,
                *[pltpu.VMEM((cells + 2 * PAD, 128), F32)] * 2,
                pltpu.VMEM((cells, 128), F32),
                *[pltpu.VMEM((6, th + 2 * PAD, 128), F32)] * 2,
                *[pltpu.VMEM((cells, 128), F32)] * 2,
                *[pltpu.VMEM((2 * th, 128), F32)] * 2,
                *[pltpu.VMEM((block[1] * tw, 768), F32) for block in (BLOCK_A, BLOCK_B, BLOCK_C, BLOCK_D)],
                pltpu.VMEM((4 * tw, 768), F32),
                pltpu.VMEM((9, c_in + c_hid, 4 * c_hid), BF16),
                pltpu.VMEM((9 * (c_in + c_hid), 4 * c_hid), BF16),
                pltpu.VMEM((cells, c_hid), BF16),
                pltpu.VMEM((cells, c_hid), F32),
                pltpu.VMEM((2, cells, c_in), BF16),
                pltpu.VMEM((4, tw, 256), BF16),
                pltpu.VMEM((2, 4, tw, 256), BF16),
                pltpu.VMEM((2, 4, tw // 2, 256), BF16),
                pltpu.SemaphoreType.DMA((8,)),
                pltpu.SemaphoreType.DMA((2, 8)),
                pltpu.SemaphoreType.DMA((2,)),
                pltpu.SemaphoreType.DMA((5,)),
            ],
            compiler_params=pltpu.CompilerParams(collective_id=0, has_side_effects=True, vmem_limit_bytes=40 << 20),
        )
        hidden, c_last = run(frames.reshape(steps, cells, c_in), w_in.reshape(9, c_in, -1), w_rec.reshape(9, c_hid, -1),
                             gate_bias.reshape(1, -1), h_init.reshape(cells, c_hid), c_init.reshape(cells, c_hid))
        return hidden.reshape(steps, 1, th, tw, c_hid), c_last.reshape(1, th, tw, c_hid)

    return jax.shard_map(local_run, mesh=mesh, in_specs=(seq_spec, P(), P(), P(), state_spec, state_spec),
                         out_specs=(seq_spec, state_spec), check_vma=False)
```

```python
import functools

import jax
import jax.numpy as jnp
from jax import lax
from jax.experimental import pallas as pl
from jax.experimental.pallas import tpu as pltpu
from jax.sharding import PartitionSpec as P

MESH = pl.DeviceIdType.MESH
BF16, F32 = jnp.bfloat16, jnp.float32
PAD = 8
PITCH = 40
UP, DOWN, LEFT, RIGHT = range(4)
UL, UR, DL, DR = range(4)
BLOCK_A, BLOCK_B, BLOCK_C, BLOCK_D = (1, 8), (9, 9), (18, 8), (26, 4)
RING_ROWS = (0, 30, 31)


def half_tanh(x):
    return 0.5 * jnp.tanh(0.5 * x) + 0.5


def kernel(n_rows, n_cols, steps, th, tw,
           frames, w_in, w_rec, gate_bias, h_hbm, c_hbm, hs, c_out,
           xm, xt, fx, em, et, cm, ct, colm, colt, ga, gb, gc, gd, gr,
           wraw, ws, hb, cb, fr, send, land, corner, send_sem, recv_sem, fr_sem, in_sem):
    row, col = lax.axis_index("rows"), lax.axis_index("cols")
    has = {UP: row > 0, DOWN: row < n_rows - 1, LEFT: col > 0, RIGHT: col < n_cols - 1}
    cells = th * tw

    def routes(slot):
        half = tw // 2
        edge = lambda place: land.at[slot, place]
        point = lambda place: corner.at[slot, place]
        return [
            (has[UP], -1, 0, send.at[UP], 0, edge(DOWN)),
            (has[DOWN], 1, 0, send.at[DOWN], 1, edge(UP)),
            (has[LEFT], 0, -1, send.at[2], 2, edge(RIGHT)),
            (has[RIGHT], 0, 1, send.at[2], 3, edge(LEFT)),
            (has[UP] & has[LEFT], -1, -1, send.at[UP, pl.ds(0, half)], 4, point(DR)),
            (has[UP] & has[RIGHT], -1, 1, send.at[UP, pl.ds(half, half)], 5, point(DL)),
            (has[DOWN] & has[LEFT], 1, -1, send.at[DOWN, pl.ds(0, half)], 6, point(UR)),
            (has[DOWN] & has[RIGHT], 1, 1, send.at[DOWN, pl.ds(half, half)], 7, point(UL)),
        ]

    def copy_of(route, slot):
        _, d_row, d_col, src, index, dst = route
        return pltpu.make_async_remote_copy(
            src_ref=src, dst_ref=dst, send_sem=send_sem.at[index], recv_sem=recv_sem.at[slot, index],
            device_id={"rows": row + d_row, "cols": col + d_col}, device_id_type=MESH)

    def start_sends(slot):
        for route in routes(slot):
            @pl.when(route[0])
            def _():
                copy_of(route, slot).start()

    def wait_sends(slot):
        for route in routes(slot):
            @pl.when(route[0])
            def _():
                copy_of(route, slot).wait_send()

    def wait_recvs(slot):
        came = [has[DOWN], has[UP], has[RIGHT], has[LEFT], has[DOWN] & has[RIGHT], has[DOWN] & has[LEFT],
                has[UP] & has[RIGHT], has[UP] & has[LEFT]]
        for route, condition in zip(routes(slot), came):
            @pl.when(condition)
            def _():
                copy_of(route, slot).wait_recv()

    def frame_copy(t, slot):
        return pltpu.make_async_copy(frames.at[jnp.minimum(t, steps - 1)], fr.at[slot], fr_sem.at[slot])

    weight_copies = [
        pltpu.make_async_copy(w_rec.at[:, pl.ds(0, 128)], wraw.at[:, pl.ds(0, 128)], in_sem.at[0]),
        pltpu.make_async_copy(w_in, wraw.at[:, pl.ds(128, 64)], in_sem.at[1]),
        pltpu.make_async_copy(w_rec.at[:, pl.ds(128, 64)], wraw.at[:, pl.ds(192, 64)], in_sem.at[2]),
    ]
    state_copies = [pltpu.make_async_copy(h_hbm, hb, in_sem.at[3]), pltpu.make_async_copy(c_hbm, cb, in_sem.at[4])]

    bias = lane_order(gate_bias[...].reshape(1, 768), 192)
    lane = lax.broadcasted_iota(jnp.int32, (tw, 128), 1)
    low = lane < 64
    scale = jnp.where(low, 1.0, 0.5)
    shift = jnp.where(low, 0.0, 0.5)
    x = (xm, xt)
    inner = (1 - col) * (tw - 1)
    edges = (em, et)
    own, beside, beyond = 1, 2 * col, 2 - 2 * col

    def base(i):
        return PAD + (i + 1) * PITCH + 8

    def row_at(i):
        return pl.ds(base(i), tw)

    def col_at(j, first=0, size=th):
        return pl.ds(base(first) + j, size, stride=PITCH)

    def dot(lhs):
        return lax.dot_general(jnp.concatenate(lhs, axis=1), ws[...], (((1,), (0,)), ((), ())), preferred_element_type=F32)

    def row_parts(rows, dy, dx):
        return [jnp.concatenate([part[pl.ds(base(i + dy - 1) + dx - 1, tw), :] for i in rows], axis=0) for part in x]

    def matmul(g_ref, block):
        rows = range(block[0], sum(block))
        g_ref[...] = dot([v for dy in range(3) for dx in range(3) for v in row_parts(rows, dy, dx)])

    def ring_matmul():
        lhs = []
        for dy in range(3):
            for dx in range(3):
                for part, value in enumerate(row_parts(RING_ROWS, dy, dx)):
                    lhs.append(jnp.concatenate([value, edges[part][dx, pl.ds(PAD - 1 + dy, th), :]], axis=0))
        gr[...] = dot(lhs)

    def cell(gates, c_main, c_tail, frame):
        pre = [gates(k) + bias[:, 128 * k:128 * (k + 1)] for k in range(6)]
        n_main = half_tanh(pre[1]) * c_main + half_tanh(pre[0]) * jnp.tanh(pre[3])
        h_main = half_tanh(pre[2]) * jnp.tanh(n_main)
        fore = half_tanh(pre[4])
        back = jnp.tanh(pre[5] * scale) * scale + shift
        n_tail = fore * c_tail + pltpu.roll(fore * back, 64, 1)
        return n_main, n_tail, h_main, jnp.where(low, frame, back * jnp.tanh(n_tail))

    def update_row(g_ref, g_row, i):
        at = pl.ds(i * tw, tw)
        cm[at, :], ct[at, :], xm[row_at(i), :], xt[row_at(i), :] = cell(
            lambda k: g_ref[pl.ds(g_row, tw), 128 * k:128 * (k + 1)], cm[at, :], ct[at, :], fx[at, :])

    def update_rows(g_ref, block, rows):
        for i in rows:
            update_row(g_ref, (i - block[0]) * tw, i)

    def update_ring():
        update_row(gr, 0, 0)
        update_row(gr, 2 * tw, th - 1)
        g_row = len(RING_ROWS) * tw
        colm[...], colt[...], *values = cell(
            lambda k: gr[pl.ds(g_row, th), 128 * k:128 * (k + 1)], colm[...], colt[...], fx[pl.ds(inner, th, stride=tw), :])
        for part, value in enumerate(values):
            edges[part][own, PAD:PAD + th, :] = value
            x[part][col_at(inner, 0, th - 8), :] = value[:th - 8]
            x[part][pl.ds(base(th - 1) + inner, 1), :] = value[th - 1:]
            send[2, :, 128 * part:128 * (part + 1)] = value.astype(BF16)
        fill_row_sends()

    def fill_row_sends():
        for place, i in ((UP, 0), (DOWN, th - 1)):
            for part in range(2):
                send[place, :, 128 * part:128 * (part + 1)] = x[part][row_at(i), :].astype(BF16)

    def keep_beside():
        for part, e in enumerate(edges):
            e[beside, PAD:PAD + th, :] = x[part][col_at(inner + 1 - beyond), :]

    def finish_step():
        update_rows(gc, BLOCK_C, [25])
        update_rows(gd, BLOCK_D, range(26, 30))
        update_row(gr, tw, 30)
        for part, e in enumerate(edges):
            x[part][col_at(inner, th - 8, 8), :] = e[own, PAD + th - 8:PAD + th, :]
        keep_beside()

    def form_out(t):
        for i in range(th):
            at = pl.ds(i * tw, tw)
            hs[t, at, 0:128] = x[0][row_at(i), :].astype(BF16)
            hs[t, at, 128:192] = pltpu.roll(x[1][row_at(i), :], 64, 1)[:, :64].astype(BF16)

    def convert_frame(slot):
        for i in range(th):
            at = pl.ds(i * tw, tw)
            fx[at, 0:64] = fr[slot, at, :].astype(F32)

    def place_halo(slot):
        for part, e in enumerate(edges):
            lanes = slice(128 * part, 128 * (part + 1))
            for place, i in ((UP, -1), (DOWN, th)):
                x[part][row_at(i), :] = land[slot, place, :, lanes].astype(F32)
            for place, i, j, r in ((UL, -1, -1, 15), (UR, -1, tw, 0), (DL, th, -1, 15), (DR, th, tw, 0)):
                x[part][pl.ds(base(i) + j, 1), :] = corner[slot, place, :, lanes].astype(F32)[r:r + 1, :]
            e[beyond, PAD:PAD + th, :] = land[slot, RIGHT - col, :, lanes].astype(F32)
            for k in range(3):
                for i in (-1, th):
                    e[k, PAD + i:PAD + i + 1, :] = x[part][pl.ds(base(i) + inner - 1 + k, 1), :]

    def late_blocks():
        ring_matmul()
        update_rows(ga, BLOCK_A, [1])
        update_rows(gb, BLOCK_B, [17])
        update_rows(gc, BLOCK_C, range(18, 25))
        matmul(gd, BLOCK_D)
        update_ring()

    def early_blocks(t, frame_slot):
        matmul(ga, BLOCK_A)
        if t is not None:
            finish_step()
            form_out(t)
        convert_frame(frame_slot)
        matmul(gb, BLOCK_B)
        update_rows(ga, BLOCK_A, range(2, 8))
        matmul(gc, BLOCK_C)
        update_rows(ga, BLOCK_A, [8])
        update_rows(gb, BLOCK_B, range(9, 17))

    for copy in state_copies:
        copy.start()
    frame_copy(0, 0).start()
    for copy in weight_copies:
        copy.start()
    frame_copy(1, 1).start()
    land[...] = jnp.zeros_like(land)
    corner[...] = jnp.zeros_like(corner)
    for ref in (em, et, xm, xt):
        ref[...] = jnp.zeros_like(ref)
    fx[...] = jnp.zeros_like(fx)

    barrier = pltpu.get_barrier_semaphore()
    neighbours = 0
    for condition, d_row, d_col, *_ in routes(0):
        neighbours = neighbours + condition.astype(jnp.int32)

        @pl.when(condition)
        def _():
            pl.semaphore_signal(barrier, inc=1, device_id={"rows": row + d_row, "cols": col + d_col}, device_id_type=MESH)
    pl.semaphore_wait(barrier, neighbours)

    frame_copy(0, 0).wait()
    for copy in state_copies:
        copy.wait()

    @pl.loop(0, th)
    def _(i):
        at = pl.ds(pl.multiple_of(i * tw, tw), tw)
        to = pl.ds(pl.multiple_of(base(0) + i * PITCH, 8), tw)
        xm[to, :] = hb[at, 0:128].astype(F32)
        tail = hb[at, 128:192].astype(F32)
        xt[to, :] = jnp.concatenate([fr[0, at, :].astype(F32), tail], axis=1)
        cm[at, :] = cb[at, 0:128]
        tail = cb[at, 128:192]
        ct[at, :] = jnp.concatenate([tail, tail], axis=1)

    colm[...] = cm[pl.ds(inner, th, stride=tw), :]
    colt[...] = ct[pl.ds(inner, th, stride=tw), :]
    for part in range(2):
        value = x[part][col_at(inner), :]
        edges[part][own, PAD:PAD + th, :] = value
        send[2, :, 128 * part:128 * (part + 1)] = value.astype(BF16)
    keep_beside()
    fill_row_sends()
    start_sends(0)
    frame_copy(1, 1).wait()
    frame_copy(2, 0).start()
    for copy in weight_copies:
        copy.wait()

    @pl.loop(0, 9)
    def _(tap):
        for k in range(0, 256, 64):
            at = pl.ds(pl.multiple_of(tap * 256 + k, 64), 64)
            ws[at, :] = lane_order(wraw[tap, k:k + 64, :], 192)
    early_blocks(None, 1)

    def arrive(slot):
        wait_recvs(slot)
        wait_sends(slot)
        place_halo(slot)

    def body(t, carry):
        slot = lax.rem(t, 2)
        frame_copy(t + 2, slot).wait()
        frame_copy(t + 3, 1 - slot).start()
        arrive(slot)
        late_blocks()
        start_sends(1 - slot)
        early_blocks(t, slot)
        return carry

    last = steps - 1
    lax.fori_loop(0, last, body, 0)
    frame_copy(last + 2, last % 2).wait()
    arrive(last % 2)
    late_blocks()
    finish_step()
    form_out(last)
    cm[pl.ds(inner, th, stride=tw), :] = colm[...]
    ct[pl.ds(inner, th, stride=tw), :] = colt[...]

    @pl.loop(0, th)
    def _(i):
        at = pl.ds(pl.multiple_of(i * tw, tw), tw)
        c_out[at, 0:128] = cm[at, :]
        c_out[at, 128:192] = pltpu.roll(ct[at, :], 64, 1)[:, :64]


def lane_order(x, c):
    i, f, o, g = (x[..., k * c:(k + 1) * c] for k in range(4))
    return jnp.concatenate([i[..., :128], f[..., :128], o[..., :128], g[..., :128],
                            i[..., 128:], f[..., 128:], g[..., 128:], o[..., 128:]], axis=-1)


def solution(mesh):
    n_rows, n_cols = mesh.shape["rows"], mesh.shape["cols"]
    seq_spec = P(None, "dp", "rows", "cols", None)
    state_spec = P("dp", "rows", "cols", None)

    def local_run(frames, w_in, w_rec, gate_bias, h_init, c_init):
        steps, _, th, tw, c_in = frames.shape
        c_hid = h_init.shape[-1]
        cells = th * tw
        vmem = pl.BlockSpec(memory_space=pltpu.VMEM)
        hbm = pl.BlockSpec(memory_space=pl.ANY)
        run = pl.pallas_call(
            functools.partial(kernel, n_rows, n_cols, steps, th, tw),
            out_shape=(pltpu.VMEM((steps, cells, c_hid), BF16), pltpu.VMEM((cells, c_hid), F32)),
            in_specs=[hbm, hbm, hbm, vmem, hbm, hbm],
            out_specs=(vmem, vmem),
            scratch_shapes=[
                *[pltpu.VMEM((PAD + (th + 2) * PITCH + PAD, 128), F32)] * 2,
                pltpu.VMEM((cells, 128), F32),
                *[pltpu.VMEM((3, th + 2 * PAD, 128), F32)] * 2,
                *[pltpu.VMEM((cells, 128), F32)] * 2,
                *[pltpu.VMEM((th, 128), F32)] * 2,
                *[pltpu.VMEM((block[1] * tw, 768), F32) for block in (BLOCK_A, BLOCK_B, BLOCK_C, BLOCK_D)],
                pltpu.VMEM(((len(RING_ROWS) + 1) * tw, 768), F32),
                pltpu.VMEM((9, c_in + c_hid, 4 * c_hid), BF16),
                pltpu.VMEM((9 * (c_in + c_hid), 4 * c_hid), BF16),
                pltpu.VMEM((cells, c_hid), BF16),
                pltpu.VMEM((cells, c_hid), F32),
                pltpu.VMEM((2, cells, c_in), BF16),
                pltpu.VMEM((4, tw, 256), BF16),
                pltpu.VMEM((2, 4, tw, 256), BF16),
                pltpu.VMEM((2, 4, tw // 2, 256), BF16),
                pltpu.SemaphoreType.DMA((8,)),
                pltpu.SemaphoreType.DMA((2, 8)),
                pltpu.SemaphoreType.DMA((2,)),
                pltpu.SemaphoreType.DMA((5,)),
            ],
            compiler_params=pltpu.CompilerParams(collective_id=0, has_side_effects=True, vmem_limit_bytes=40 << 20),
        )
        hidden, c_last = run(frames.reshape(steps, cells, c_in), w_in.reshape(9, c_in, -1), w_rec.reshape(9, c_hid, -1),
                             gate_bias, h_init.reshape(cells, c_hid), c_init.reshape(cells, c_hid))
        return hidden.reshape(steps, 1, th, tw, c_hid), c_last.reshape(1, th, tw, c_hid)

    return jax.shard_map(local_run, mesh=mesh, in_specs=(seq_spec, P(), P(), P(), state_spec, state_spec),
                         out_specs=(seq_spec, state_spec), check_vma=False)
```

```python
import functools

import jax
import jax.numpy as jnp
from jax import lax
from jax.experimental import pallas as pl
from jax.experimental.pallas import tpu as pltpu
from jax.sharding import PartitionSpec as P

MESH = pl.DeviceIdType.MESH
BF16, F32 = jnp.bfloat16, jnp.float32
PAD = 8
PITCH = 40
UP, DOWN, SIDE = range(3)
BLOCK_A, BLOCK_B, BLOCK_C, BLOCK_D = (1, 8), (9, 9), (18, 8), (26, 4)
RING_ROWS = (0, 30, 31)


def half_tanh(x):
    return 0.5 * jnp.tanh(0.5 * x) + 0.5


def kernel(n_rows, n_cols, steps, th, tw,
           frames, w_in, w_rec, gate_bias, h_hbm, c_hbm, hs, c_out,
           xm, xt, fx, em, et, cm, ct, colm, colt, ga, gb, gc, gd, gr,
           wraw, ws, hb, cb, fr, send, land, corner, send_sem, recv_sem, fr_sem, in_sem):
    row, col = lax.axis_index("rows"), lax.axis_index("cols")
    above, below = row > 0, row < n_rows - 1
    cells = th * tw
    half = tw // 2
    near = pl.ds(pl.multiple_of((1 - col) * half, half), half)

    def routes(slot):
        across = 1 - 2 * col
        return [
            (above, -1, 0, send.at[UP], land.at[slot, DOWN]),
            (below, 1, 0, send.at[DOWN], land.at[slot, UP]),
            (None, 0, across, send.at[SIDE], land.at[slot, SIDE]),
            (above, -1, across, send.at[UP, near], corner.at[slot, DOWN]),
            (below, 1, across, send.at[DOWN, near], corner.at[slot, UP]),
        ]

    def guarded(condition, run):
        run() if condition is None else pl.when(condition)(run)

    def copies(slot):
        for index, (condition, d_row, d_col, src, dst) in enumerate(routes(slot)):
            yield condition, pltpu.make_async_remote_copy(
                src_ref=src, dst_ref=dst, send_sem=send_sem.at[index], recv_sem=recv_sem.at[slot, index],
                device_id={"rows": row + d_row, "cols": col + d_col}, device_id_type=MESH)

    def start_sends(slot):
        for condition, copy in copies(slot):
            guarded(condition, copy.start)

    def wait_sends(slot):
        for condition, copy in copies(slot):
            guarded(condition, copy.wait_send)

    def wait_recvs(slot):
        for came, (_, copy) in zip((below, above, None, below, above), copies(slot)):
            guarded(came, copy.wait_recv)

    def frame_copy(t, slot):
        return pltpu.make_async_copy(frames.at[jnp.minimum(t, steps - 1)], fr.at[slot], fr_sem.at[slot])

    weight_copies = [
        pltpu.make_async_copy(w_rec.at[:, pl.ds(0, 128)], wraw.at[:, pl.ds(0, 128)], in_sem.at[0]),
        pltpu.make_async_copy(w_in, wraw.at[:, pl.ds(128, 64)], in_sem.at[1]),
        pltpu.make_async_copy(w_rec.at[:, pl.ds(128, 64)], wraw.at[:, pl.ds(192, 64)], in_sem.at[2]),
    ]
    state_copies = [pltpu.make_async_copy(h_hbm, hb, in_sem.at[3]), pltpu.make_async_copy(c_hbm, cb, in_sem.at[4])]

    bias = lane_order(gate_bias[...].reshape(1, 768), 192)
    lane = lax.broadcasted_iota(jnp.int32, (tw, 128), 1)
    low = lane < 64
    scale = jnp.where(low, 1.0, 0.5)
    shift = jnp.where(low, 0.0, 0.5)
    x = (xm, xt)
    inner = (1 - col) * (tw - 1)
    edges = (em, et)
    own, beside, beyond = 1, 2 * col, 2 - 2 * col

    def base(i):
        return PAD + (i + 1) * PITCH + 8

    def row_at(i):
        return pl.ds(base(i), tw)

    def col_at(j, first=0, size=th):
        return pl.ds(base(first) + j, size, stride=PITCH)

    def dot(lhs):
        return lax.dot_general(jnp.concatenate(lhs, axis=1), ws[...], (((1,), (0,)), ((), ())), preferred_element_type=F32)

    def row_parts(rows, dy, dx):
        return [jnp.concatenate([part[pl.ds(base(i + dy - 1) + dx - 1, tw), :] for i in rows], axis=0) for part in x]

    def matmul(g_ref, block):
        rows = range(block[0], sum(block))
        g_ref[...] = dot([v for dy in range(3) for dx in range(3) for v in row_parts(rows, dy, dx)])

    def ring_matmul():
        lhs = []
        for dy in range(3):
            for dx in range(3):
                for part, value in enumerate(row_parts(RING_ROWS, dy, dx)):
                    lhs.append(jnp.concatenate([value, edges[part][dx, pl.ds(PAD - 1 + dy, th), :]], axis=0))
        gr[...] = dot(lhs)

    def cell(gates, c_main, c_tail, frame):
        pre = [gates(k) + bias[:, 128 * k:128 * (k + 1)] for k in range(6)]
        n_main = half_tanh(pre[1]) * c_main + half_tanh(pre[0]) * jnp.tanh(pre[3])
        h_main = half_tanh(pre[2]) * jnp.tanh(n_main)
        fore = half_tanh(pre[4])
        back = jnp.tanh(pre[5] * scale) * scale + shift
        n_tail = fore * c_tail + pltpu.roll(fore * back, 64, 1)
        return n_main, n_tail, h_main, jnp.where(low, frame, back * jnp.tanh(n_tail))

    def update_row(g_ref, g_row, i):
        at = pl.ds(i * tw, tw)
        cm[at, :], ct[at, :], xm[row_at(i), :], xt[row_at(i), :] = cell(
            lambda k: g_ref[pl.ds(g_row, tw), 128 * k:128 * (k + 1)], cm[at, :], ct[at, :], fx[at, :])

    def update_rows(g_ref, block, rows):
        for i in rows:
            update_row(g_ref, (i - block[0]) * tw, i)

    def update_ring():
        update_row(gr, 0, 0)
        update_row(gr, 2 * tw, th - 1)
        g_row = len(RING_ROWS) * tw
        colm[...], colt[...], *values = cell(
            lambda k: gr[pl.ds(g_row, th), 128 * k:128 * (k + 1)], colm[...], colt[...], fx[pl.ds(inner, th, stride=tw), :])
        for part, value in enumerate(values):
            edges[part][own, PAD:PAD + th, :] = value
            x[part][col_at(inner, 0, th - 8), :] = value[:th - 8]
            x[part][pl.ds(base(th - 1) + inner, 1), :] = value[th - 1:]
            send[SIDE, :, 128 * part:128 * (part + 1)] = value.astype(BF16)
        fill_row_sends()

    def fill_row_sends():
        for place, i in ((UP, 0), (DOWN, th - 1)):
            for part in range(2):
                send[place, :, 128 * part:128 * (part + 1)] = x[part][row_at(i), :].astype(BF16)

    def keep_beside():
        for part, e in enumerate(edges):
            e[beside, PAD:PAD + th, :] = x[part][col_at(inner + 1 - beyond), :]

    def finish_step():
        update_rows(gc, BLOCK_C, [25])
        update_rows(gd, BLOCK_D, range(26, 30))
        update_row(gr, tw, 30)
        for part, e in enumerate(edges):
            x[part][col_at(inner, th - 8, 8), :] = e[own, PAD + th - 8:PAD + th, :]
        keep_beside()

    def form_out(t):
        for i in range(th):
            at = pl.ds(i * tw, tw)
            hs[t, at, 0:128] = x[0][row_at(i), :].astype(BF16)
            hs[t, at, 128:192] = pltpu.roll(x[1][row_at(i), :], 64, 1)[:, :64].astype(BF16)

    def convert_frame(slot):
        for i in range(th):
            at = pl.ds(i * tw, tw)
            fx[at, 0:64] = fr[slot, at, :].astype(F32)

    def place_halo(slot):
        for part, e in enumerate(edges):
            lanes = slice(128 * part, 128 * (part + 1))
            for place, i in ((UP, -1), (DOWN, th)):
                x[part][row_at(i), :] = land[slot, place, :, lanes].astype(F32)
                value = corner[slot, place, :, lanes].astype(F32)
                value = jnp.where(col == 0, value[0:1, :], value[half - 1:, :])
                x[part][pl.ds(base(i) + inner + 1 - 2 * col, 1), :] = value
            e[beyond, PAD:PAD + th, :] = land[slot, SIDE, :, lanes].astype(F32)
            for k in range(3):
                for i in (-1, th):
                    e[k, PAD + i:PAD + i + 1, :] = x[part][pl.ds(base(i) + inner - 1 + k, 1), :]

    def late_blocks():
        ring_matmul()
        update_rows(ga, BLOCK_A, [1])
        update_rows(gb, BLOCK_B, [17])
        update_rows(gc, BLOCK_C, range(18, 25))
        matmul(gd, BLOCK_D)
        update_ring()

    def early_blocks(t, frame_slot):
        matmul(ga, BLOCK_A)
        if t is not None:
            finish_step()
            form_out(t)
        convert_frame(frame_slot)
        matmul(gb, BLOCK_B)
        update_rows(ga, BLOCK_A, range(2, 8))
        matmul(gc, BLOCK_C)
        update_rows(ga, BLOCK_A, [8])
        update_rows(gb, BLOCK_B, range(9, 17))

    for copy in state_copies:
        copy.start()
    frame_copy(0, 0).start()
    for copy in weight_copies:
        copy.start()
    frame_copy(1, 1).start()
    land[...] = jnp.zeros_like(land)
    corner[...] = jnp.zeros_like(corner)
    barrier = pltpu.get_barrier_semaphore()
    neighbours = 1 + 2 * above.astype(jnp.int32) + 2 * below.astype(jnp.int32)
    for condition, d_row, d_col, *_ in routes(0):
        guarded(condition, functools.partial(
            pl.semaphore_signal, barrier, inc=1, device_id={"rows": row + d_row, "cols": col + d_col}, device_id_type=MESH))
    for ref in (em, et, xm, xt):
        ref[...] = jnp.zeros_like(ref)
    fx[...] = jnp.zeros_like(fx)

    frame_copy(0, 0).wait()
    for copy in state_copies:
        copy.wait()

    @pl.loop(0, th, step=8)
    def _(first):
        for k in range(8):
            i = first + k
            at = pl.ds(pl.multiple_of(i * tw, tw), tw)
            to = pl.ds(pl.multiple_of(base(0) + i * PITCH, 8), tw)
            xm[to, :] = hb[at, 0:128].astype(F32)
            tail = hb[at, 128:192].astype(F32)
            xt[to, :] = jnp.concatenate([fr[0, at, :].astype(F32), tail], axis=1)
            cm[at, :] = cb[at, 0:128]
            tail = cb[at, 128:192]
            ct[at, :] = jnp.concatenate([tail, tail], axis=1)

    colm[...] = cm[pl.ds(inner, th, stride=tw), :]
    colt[...] = ct[pl.ds(inner, th, stride=tw), :]
    for part in range(2):
        value = x[part][col_at(inner), :]
        edges[part][own, PAD:PAD + th, :] = value
        send[SIDE, :, 128 * part:128 * (part + 1)] = value.astype(BF16)
    keep_beside()
    fill_row_sends()
    pl.semaphore_wait(barrier, neighbours)
    start_sends(0)
    frame_copy(1, 1).wait()
    frame_copy(2, 0).start()
    for copy in weight_copies:
        copy.wait()

    @pl.loop(0, 9)
    def _(tap):
        for k in range(0, 256, 64):
            at = pl.ds(pl.multiple_of(tap * 256 + k, 64), 64)
            ws[at, :] = lane_order(wraw[tap, k:k + 64, :], 192)
    early_blocks(None, 1)

    def arrive(slot):
        wait_recvs(slot)
        wait_sends(slot)
        place_halo(slot)

    def body(t, carry):
        slot = lax.rem(t, 2)
        frame_copy(t + 2, slot).wait()
        frame_copy(t + 3, 1 - slot).start()
        arrive(slot)
        late_blocks()
        start_sends(1 - slot)
        early_blocks(t, slot)
        return carry

    last = steps - 1
    lax.fori_loop(0, last, body, 0)
    frame_copy(last + 2, last % 2).wait()
    arrive(last % 2)
    late_blocks()
    finish_step()
    form_out(last)
    cm[pl.ds(inner, th, stride=tw), :] = colm[...]
    ct[pl.ds(inner, th, stride=tw), :] = colt[...]

    for i in range(th):
        at = pl.ds(i * tw, tw)
        c_out[at, 0:128] = cm[at, :]
        c_out[at, 128:192] = pltpu.roll(ct[at, :], 64, 1)[:, :64]


def write_kernel(hs, c, hs_hbm, c_hbm, sems):
    copies = [pltpu.make_async_copy(hs.at[t], hs_hbm.at[t], sems.at[t]) for t in range(hs.shape[0])]
    copies.append(pltpu.make_async_copy(c, c_hbm, sems.at[hs.shape[0]]))
    for copy in copies:
        copy.start()
    for copy in copies:
        copy.wait()


def lane_order(x, c):
    i, f, o, g = (x[..., k * c:(k + 1) * c] for k in range(4))
    return jnp.concatenate([i[..., :128], f[..., :128], o[..., :128], g[..., :128],
                            i[..., 128:], f[..., 128:], g[..., 128:], o[..., 128:]], axis=-1)


def solution(mesh):
    n_rows, n_cols = mesh.shape["rows"], mesh.shape["cols"]
    seq_spec = P(None, "dp", "rows", "cols", None)
    state_spec = P("dp", "rows", "cols", None)

    def local_run(frames, w_in, w_rec, gate_bias, h_init, c_init):
        steps, _, th, tw, c_in = frames.shape
        c_hid = h_init.shape[-1]
        cells = th * tw
        vmem = pl.BlockSpec(memory_space=pltpu.VMEM)
        hbm = pl.BlockSpec(memory_space=pl.ANY)
        run = pl.pallas_call(
            functools.partial(kernel, n_rows, n_cols, steps, th, tw),
            out_shape=(pltpu.VMEM((steps, cells, c_hid), BF16), pltpu.VMEM((cells, c_hid), F32)),
            in_specs=[hbm, hbm, hbm, vmem, hbm, hbm],
            out_specs=(vmem, vmem),
            scratch_shapes=[
                *[pltpu.VMEM((PAD + (th + 2) * PITCH + PAD, 128), F32)] * 2,
                pltpu.VMEM((cells, 128), F32),
                *[pltpu.VMEM((3, th + 2 * PAD, 128), F32)] * 2,
                *[pltpu.VMEM((cells, 128), F32)] * 2,
                *[pltpu.VMEM((th, 128), F32)] * 2,
                *[pltpu.VMEM((block[1] * tw, 768), F32) for block in (BLOCK_A, BLOCK_B, BLOCK_C, BLOCK_D)],
                pltpu.VMEM(((len(RING_ROWS) + 1) * tw, 768), F32),
                pltpu.VMEM((9, c_in + c_hid, 4 * c_hid), BF16),
                pltpu.VMEM((9 * (c_in + c_hid), 4 * c_hid), BF16),
                pltpu.VMEM((cells, c_hid), BF16),
                pltpu.VMEM((cells, c_hid), F32),
                pltpu.VMEM((2, cells, c_in), BF16),
                pltpu.VMEM((3, tw, 256), BF16),
                pltpu.VMEM((2, 3, tw, 256), BF16),
                pltpu.VMEM((2, 2, tw // 2, 256), BF16),
                pltpu.SemaphoreType.DMA((5,)),
                pltpu.SemaphoreType.DMA((2, 5)),
                pltpu.SemaphoreType.DMA((2,)),
                pltpu.SemaphoreType.DMA((5,)),
            ],
            compiler_params=pltpu.CompilerParams(collective_id=0, has_side_effects=True, vmem_limit_bytes=40 << 20),
        )
        hidden, c_last = run(frames.reshape(steps, cells, c_in), w_in.reshape(9, c_in, -1), w_rec.reshape(9, c_hid, -1),
                             gate_bias, h_init.reshape(cells, c_hid), c_init.reshape(cells, c_hid))
        hidden, c_last = pl.pallas_call(
            write_kernel,
            out_shape=(jax.ShapeDtypeStruct(hidden.shape, BF16), jax.ShapeDtypeStruct(c_last.shape, F32)),
            in_specs=[vmem, vmem],
            out_specs=(hbm, hbm),
            scratch_shapes=[pltpu.SemaphoreType.DMA((steps + 1,))],
            compiler_params=pltpu.CompilerParams(vmem_limit_bytes=1 << 20),
        )(hidden, c_last)
        return hidden.reshape(steps, 1, th, tw, c_hid), c_last.reshape(1, th, tw, c_hid)

    return jax.shard_map(local_run, mesh=mesh, in_specs=(seq_spec, P(), P(), P(), state_spec, state_spec),
                         out_specs=(seq_spec, state_spec), check_vma=False)
```

```python
import functools

import jax
import jax.numpy as jnp
from jax import lax
from jax.experimental import pallas as pl
from jax.experimental.pallas import tpu as pltpu
from jax.sharding import PartitionSpec as P

MESH = pl.DeviceIdType.MESH
BF16, F32 = jnp.bfloat16, jnp.float32
PAD = 8
PITCH = 40
UP, DOWN, SIDE = range(3)
BLOCK_A, BLOCK_B, BLOCK_C, BLOCK_D = (1, 10), (11, 10), (21, 5), (26, 4)
RING_ROWS = (0, 30, 31)


def half_tanh(x):
    return 0.5 * jnp.tanh(0.5 * x) + 0.5


def kernel(n_rows, n_cols, steps, th, tw,
           frames, w_in, w_rec, gate_bias, h_hbm, c_hbm, hs, c_out,
           xm, xt, fx, em, et, cm, ct, colm, colt, ga, gb, gc, gd, gr,
           wraw, ws, hb, cb, fr, send, land, corner, send_sem, recv_sem, fr_sem, in_sem):
    row, col = lax.axis_index("rows"), lax.axis_index("cols")
    above, below = row > 0, row < n_rows - 1
    cells = th * tw
    half = tw // 2
    near = pl.ds(pl.multiple_of((1 - col) * half, half), half)

    def routes(slot):
        across = 1 - 2 * col
        return [
            (above, -1, 0, send.at[UP], land.at[slot, DOWN]),
            (below, 1, 0, send.at[DOWN], land.at[slot, UP]),
            (None, 0, across, send.at[SIDE], land.at[slot, SIDE]),
            (above, -1, across, send.at[UP, near], corner.at[slot, DOWN]),
            (below, 1, across, send.at[DOWN, near], corner.at[slot, UP]),
        ]

    def guarded(condition, run):
        run() if condition is None else pl.when(condition)(run)

    def copies(slot):
        for index, (condition, d_row, d_col, src, dst) in enumerate(routes(slot)):
            yield condition, pltpu.make_async_remote_copy(
                src_ref=src, dst_ref=dst, send_sem=send_sem.at[index], recv_sem=recv_sem.at[slot, index],
                device_id={"rows": row + d_row, "cols": col + d_col}, device_id_type=MESH)

    def start_sends(slot):
        for condition, copy in copies(slot):
            guarded(condition, copy.start)

    def wait_sends(slot):
        for condition, copy in copies(slot):
            guarded(condition, copy.wait_send)

    def wait_recvs(slot):
        for came, (_, copy) in zip((below, above, None, below, above), copies(slot)):
            guarded(came, copy.wait_recv)

    def frame_copy(t, slot):
        return pltpu.make_async_copy(frames.at[jnp.minimum(t, steps - 1)], fr.at[slot], fr_sem.at[slot])

    weight_copies = []
    for k in range(3):
        taps = pl.ds(3 * k, 3)
        weight_copies.append([
            pltpu.make_async_copy(w_rec.at[taps, pl.ds(0, 128)], wraw.at[taps, pl.ds(0, 128)], in_sem.at[2 + 3 * k]),
            pltpu.make_async_copy(w_in.at[taps], wraw.at[taps, pl.ds(128, 64)], in_sem.at[3 + 3 * k]),
            pltpu.make_async_copy(w_rec.at[taps, pl.ds(128, 64)], wraw.at[taps, pl.ds(192, 64)], in_sem.at[4 + 3 * k]),
        ])
    state_copies = [pltpu.make_async_copy(h_hbm, hb, in_sem.at[0]), pltpu.make_async_copy(c_hbm, cb, in_sem.at[1])]

    bias = lane_order(gate_bias[...].reshape(1, 768), 192)
    lane = lax.broadcasted_iota(jnp.int32, (tw, 128), 1)
    low = lane < 64
    scale = jnp.where(low, 1.0, 0.5)
    shift = jnp.where(low, 0.0, 0.5)
    x = (xm, xt)
    inner = (1 - col) * (tw - 1)
    edges = (em, et)
    own, beside, beyond = 1, 2 * col, 2 - 2 * col

    def base(i):
        return PAD + (i + 1) * PITCH + 8

    def row_at(i):
        return pl.ds(base(i), tw)

    def col_at(j, first=0, size=th):
        return pl.ds(base(first) + j, size, stride=PITCH)

    def dot(lhs):
        return lax.dot_general(jnp.concatenate(lhs, axis=1), ws[...], (((1,), (0,)), ((), ())), preferred_element_type=F32)

    def row_parts(rows, dy, dx):
        return [jnp.concatenate([part[pl.ds(base(i + dy - 1) + dx - 1, tw), :] for i in rows], axis=0) for part in x]

    def matmul(g_ref, block):
        rows = range(block[0], sum(block))
        g_ref[...] = dot([v for dy in range(3) for dx in range(3) for v in row_parts(rows, dy, dx)])

    def ring_matmul():
        lhs = []
        for dy in range(3):
            for dx in range(3):
                for part, value in enumerate(row_parts(RING_ROWS, dy, dx)):
                    lhs.append(jnp.concatenate([value, edges[part][dx, pl.ds(PAD - 1 + dy, th), :]], axis=0))
        gr[...] = dot(lhs)

    def cell(gates, c_main, c_tail, frame):
        pre = [gates(k) + bias[:, 128 * k:128 * (k + 1)] for k in range(6)]
        n_main = half_tanh(pre[1]) * c_main + half_tanh(pre[0]) * jnp.tanh(pre[3])
        h_main = half_tanh(pre[2]) * jnp.tanh(n_main)
        fore = half_tanh(pre[4])
        back = jnp.tanh(pre[5] * scale) * scale + shift
        n_tail = fore * c_tail + pltpu.roll(fore * back, 64, 1)
        return n_main, n_tail, h_main, jnp.where(low, frame, back * jnp.tanh(n_tail))

    def update_row(g_ref, g_row, i):
        at = pl.ds(i * tw, tw)
        cm[at, :], ct[at, :], xm[row_at(i), :], xt[row_at(i), :] = cell(
            lambda k: g_ref[pl.ds(g_row, tw), 128 * k:128 * (k + 1)], cm[at, :], ct[at, :], fx[at, :])

    def update_rows(g_ref, block, rows):
        for i in rows:
            update_row(g_ref, (i - block[0]) * tw, i)

    def update_ring():
        update_row(gr, 0, 0)
        update_row(gr, 2 * tw, th - 1)
        g_row = len(RING_ROWS) * tw
        colm[...], colt[...], *values = cell(
            lambda k: gr[pl.ds(g_row, th), 128 * k:128 * (k + 1)], colm[...], colt[...], fx[pl.ds(inner, th, stride=tw), :])
        for part, value in enumerate(values):
            edges[part][own, PAD:PAD + th, :] = value
            x[part][col_at(inner, 0, th - 8), :] = value[:th - 8]
            x[part][pl.ds(base(th - 1) + inner, 1), :] = value[th - 1:]
            send[SIDE, :, 128 * part:128 * (part + 1)] = value.astype(BF16)
        fill_row_sends()

    def fill_row_sends():
        for place, i in ((UP, 0), (DOWN, th - 1)):
            for part in range(2):
                send[place, :, 128 * part:128 * (part + 1)] = x[part][row_at(i), :].astype(BF16)

    def keep_beside():
        for part, e in enumerate(edges):
            e[beside, PAD:PAD + th, :] = x[part][col_at(inner + 1 - beyond), :]

    def finish_step():
        update_rows(gc, BLOCK_C, [sum(BLOCK_C) - 1])
        update_rows(gd, BLOCK_D, range(BLOCK_D[0], sum(BLOCK_D)))
        update_row(gr, tw, 30)
        for part, e in enumerate(edges):
            x[part][col_at(inner, th - 8, 8), :] = e[own, PAD + th - 8:PAD + th, :]
        keep_beside()

    def form_out(t):
        for i in range(th):
            at = pl.ds(i * tw, tw)
            hs[t, at, 0:128] = x[0][row_at(i), :].astype(BF16)
            hs[t, at, 128:192] = pltpu.roll(x[1][row_at(i), :], 64, 1)[:, :64].astype(BF16)

    def convert_frame(slot):
        for i in range(th):
            at = pl.ds(i * tw, tw)
            fx[at, 0:64] = fr[slot, at, :].astype(F32)

    def place_halo(slot):
        for part, e in enumerate(edges):
            lanes = slice(128 * part, 128 * (part + 1))
            for place, i in ((UP, -1), (DOWN, th)):
                x[part][row_at(i), :] = land[slot, place, :, lanes].astype(F32)
                value = corner[slot, place, :, lanes].astype(F32)
                value = jnp.where(col == 0, value[0:1, :], value[half - 1:, :])
                x[part][pl.ds(base(i) + inner + 1 - 2 * col, 1), :] = value
            e[beyond, PAD:PAD + th, :] = land[slot, SIDE, :, lanes].astype(F32)
            for k in range(3):
                for i in (-1, th):
                    e[k, PAD + i:PAD + i + 1, :] = x[part][pl.ds(base(i) + inner - 1 + k, 1), :]

    def late_blocks():
        ring_matmul()
        update_rows(ga, BLOCK_A, [1])
        update_rows(gb, BLOCK_B, [sum(BLOCK_B) - 1])
        update_rows(gc, BLOCK_C, range(BLOCK_C[0], sum(BLOCK_C) - 1))
        matmul(gd, BLOCK_D)
        update_ring()

    def early_blocks(t, frame_slot):
        matmul(ga, BLOCK_A)
        if t is not None:
            finish_step()
            form_out(t)
        convert_frame(frame_slot)
        matmul(gb, BLOCK_B)
        update_rows(ga, BLOCK_A, range(2, sum(BLOCK_A) - 1))
        matmul(gc, BLOCK_C)
        update_rows(ga, BLOCK_A, [sum(BLOCK_A) - 1])
        update_rows(gb, BLOCK_B, range(BLOCK_B[0], sum(BLOCK_B) - 1))

    for copy in sum(weight_copies, []):
        copy.start()
    frame_copy(0, 0).start()
    for copy in state_copies:
        copy.start()
    frame_copy(1, 1).start()
    land[...] = jnp.zeros_like(land)
    corner[...] = jnp.zeros_like(corner)
    barrier = pltpu.get_barrier_semaphore()
    neighbours = 1 + 2 * above.astype(jnp.int32) + 2 * below.astype(jnp.int32)
    for condition, d_row, d_col, *_ in routes(0):
        guarded(condition, functools.partial(
            pl.semaphore_signal, barrier, inc=1, device_id={"rows": row + d_row, "cols": col + d_col}, device_id_type=MESH))
    for ref in (em, et, xm, xt):
        ref[...] = jnp.zeros_like(ref)
    fx[...] = jnp.zeros_like(fx)

    for k, chunk in enumerate(weight_copies):
        for copy in chunk:
            copy.wait()

        @pl.loop(3 * k, 3 * k + 3)
        def _(tap):
            for first in range(0, 256, 64):
                at = pl.ds(pl.multiple_of(tap * 256 + first, 64), 64)
                ws[at, :] = lane_order(wraw[tap, first:first + 64, :], 192)
    frame_copy(0, 0).wait()
    for copy in state_copies:
        copy.wait()

    @pl.loop(0, th, step=8)
    def _(first):
        for k in range(8):
            i = first + k
            at = pl.ds(pl.multiple_of(i * tw, tw), tw)
            to = pl.ds(pl.multiple_of(base(0) + i * PITCH, 8), tw)
            xm[to, :] = hb[at, 0:128].astype(F32)
            tail = hb[at, 128:192].astype(F32)
            xt[to, :] = jnp.concatenate([fr[0, at, :].astype(F32), tail], axis=1)
            cm[at, :] = cb[at, 0:128]
            tail = cb[at, 128:192]
            ct[at, :] = jnp.concatenate([tail, tail], axis=1)

    colm[...] = cm[pl.ds(inner, th, stride=tw), :]
    colt[...] = ct[pl.ds(inner, th, stride=tw), :]
    for part in range(2):
        value = x[part][col_at(inner), :]
        edges[part][own, PAD:PAD + th, :] = value
        send[SIDE, :, 128 * part:128 * (part + 1)] = value.astype(BF16)
    keep_beside()
    fill_row_sends()
    pl.semaphore_wait(barrier, neighbours)
    start_sends(0)
    frame_copy(1, 1).wait()
    frame_copy(2, 0).start()
    early_blocks(None, 1)

    def arrive(slot):
        wait_recvs(slot)
        wait_sends(slot)
        place_halo(slot)

    def body(t, carry):
        slot = lax.rem(t, 2)
        frame_copy(t + 2, slot).wait()
        frame_copy(t + 3, 1 - slot).start()
        arrive(slot)
        late_blocks()
        start_sends(1 - slot)
        early_blocks(t, slot)
        return carry

    last = steps - 1
    lax.fori_loop(0, last, body, 0)
    frame_copy(last + 2, last % 2).wait()
    arrive(last % 2)
    late_blocks()
    finish_step()
    form_out(last)
    cm[pl.ds(inner, th, stride=tw), :] = colm[...]
    ct[pl.ds(inner, th, stride=tw), :] = colt[...]

    for i in range(th):
        at = pl.ds(i * tw, tw)
        c_out[at, 0:128] = cm[at, :]
        c_out[at, 128:192] = pltpu.roll(ct[at, :], 64, 1)[:, :64]


def write_kernel(hs, c, hs_hbm, c_hbm, sems):
    copies = [pltpu.make_async_copy(hs.at[t], hs_hbm.at[t], sems.at[t]) for t in range(hs.shape[0])]
    copies.append(pltpu.make_async_copy(c, c_hbm, sems.at[hs.shape[0]]))
    for copy in copies:
        copy.start()
    for copy in copies:
        copy.wait()


def lane_order(x, c):
    i, f, o, g = (x[..., k * c:(k + 1) * c] for k in range(4))
    return jnp.concatenate([i[..., :128], f[..., :128], o[..., :128], g[..., :128],
                            i[..., 128:], f[..., 128:], g[..., 128:], o[..., 128:]], axis=-1)


def solution(mesh):
    n_rows, n_cols = mesh.shape["rows"], mesh.shape["cols"]
    seq_spec = P(None, "dp", "rows", "cols", None)
    state_spec = P("dp", "rows", "cols", None)

    def local_run(frames, w_in, w_rec, gate_bias, h_init, c_init):
        steps, _, th, tw, c_in = frames.shape
        c_hid = h_init.shape[-1]
        cells = th * tw
        vmem = pl.BlockSpec(memory_space=pltpu.VMEM)
        hbm = pl.BlockSpec(memory_space=pl.ANY)
        run = pl.pallas_call(
            functools.partial(kernel, n_rows, n_cols, steps, th, tw),
            out_shape=(pltpu.VMEM((steps, cells, c_hid), BF16), pltpu.VMEM((cells, c_hid), F32)),
            in_specs=[hbm, hbm, hbm, vmem, hbm, hbm],
            out_specs=(vmem, vmem),
            scratch_shapes=[
                *[pltpu.VMEM((PAD + (th + 2) * PITCH + PAD, 128), F32)] * 2,
                pltpu.VMEM((cells, 128), F32),
                *[pltpu.VMEM((3, th + 2 * PAD, 128), F32)] * 2,
                *[pltpu.VMEM((cells, 128), F32)] * 2,
                *[pltpu.VMEM((th, 128), F32)] * 2,
                *[pltpu.VMEM((block[1] * tw, 768), F32) for block in (BLOCK_A, BLOCK_B, BLOCK_C, BLOCK_D)],
                pltpu.VMEM(((len(RING_ROWS) + 1) * tw, 768), F32),
                pltpu.VMEM((9, c_in + c_hid, 4 * c_hid), BF16),
                pltpu.VMEM((9 * (c_in + c_hid), 4 * c_hid), BF16),
                pltpu.VMEM((cells, c_hid), BF16),
                pltpu.VMEM((cells, c_hid), F32),
                pltpu.VMEM((2, cells, c_in), BF16),
                pltpu.VMEM((3, tw, 256), BF16),
                pltpu.VMEM((2, 3, tw, 256), BF16),
                pltpu.VMEM((2, 2, tw // 2, 256), BF16),
                pltpu.SemaphoreType.DMA((5,)),
                pltpu.SemaphoreType.DMA((2, 5)),
                pltpu.SemaphoreType.DMA((2,)),
                pltpu.SemaphoreType.DMA((11,)),
            ],
            compiler_params=pltpu.CompilerParams(collective_id=0, has_side_effects=True, vmem_limit_bytes=40 << 20),
        )
        hidden, c_last = run(frames.reshape(steps, cells, c_in), w_in.reshape(9, c_in, -1), w_rec.reshape(9, c_hid, -1),
                             gate_bias, h_init.reshape(cells, c_hid), c_init.reshape(cells, c_hid))
        hidden, c_last = pl.pallas_call(
            write_kernel,
            out_shape=(jax.ShapeDtypeStruct(hidden.shape, BF16), jax.ShapeDtypeStruct(c_last.shape, F32)),
            in_specs=[vmem, vmem],
            out_specs=(hbm, hbm),
            scratch_shapes=[pltpu.SemaphoreType.DMA((steps + 1,))],
            compiler_params=pltpu.CompilerParams(vmem_limit_bytes=1 << 20),
        )(hidden, c_last)
        return hidden.reshape(steps, 1, th, tw, c_hid), c_last.reshape(1, th, tw, c_hid)

    return jax.shard_map(local_run, mesh=mesh, in_specs=(seq_spec, P(), P(), P(), state_spec, state_spec),
                         out_specs=(seq_spec, state_spec), check_vma=False)
```

```python
import functools

import jax
import jax.numpy as jnp
from jax import lax
from jax.experimental import pallas as pl
from jax.experimental.pallas import tpu as pltpu
from jax.sharding import PartitionSpec as P

MESH = pl.DeviceIdType.MESH
BF16, F32 = jnp.bfloat16, jnp.float32
PAD = 8
PITCH = 40
UP, DOWN, SIDE = range(3)
BLOCK_A, BLOCK_B, BLOCK_C, BLOCK_D = (1, 10), (11, 10), (21, 5), (26, 4)
RING_ROWS = (0, 30, 31)


def half_tanh(x):
    return 0.5 * jnp.tanh(0.5 * x) + 0.5


def kernel(n_rows, n_cols, steps, th, tw,
           frames, w_in, w_rec, gate_bias, h_hbm, c_hbm, hs, c_out,
           xm, xt, fx, em, et, cm, ct, colm, colt, ga, gb, gc, gd, gr,
           wraw, ws, hb, cb, fr, send, land, corner, send_sem, recv_sem, fr_sem, in_sem):
    row, col = lax.axis_index("rows"), lax.axis_index("cols")
    above, below = row > 0, row < n_rows - 1
    cells = th * tw
    half = tw // 2
    near = pl.ds(pl.multiple_of((1 - col) * half, half), half)

    def routes(slot):
        across = 1 - 2 * col
        return [
            (above, -1, 0, send.at[UP], land.at[slot, DOWN]),
            (below, 1, 0, send.at[DOWN], land.at[slot, UP]),
            (None, 0, across, send.at[SIDE], land.at[slot, SIDE]),
            (above, -1, across, send.at[UP, near], corner.at[slot, DOWN]),
            (below, 1, across, send.at[DOWN, near], corner.at[slot, UP]),
        ]

    def guarded(condition, run):
        run() if condition is None else pl.when(condition)(run)

    def copies(slot):
        for index, (condition, d_row, d_col, src, dst) in enumerate(routes(slot)):
            yield condition, pltpu.make_async_remote_copy(
                src_ref=src, dst_ref=dst, send_sem=send_sem.at[index], recv_sem=recv_sem.at[slot, index],
                device_id={"rows": row + d_row, "cols": col + d_col}, device_id_type=MESH)

    def start_sends(slot):
        for condition, copy in copies(slot):
            guarded(condition, copy.start)

    def wait_sends(slot):
        for condition, copy in copies(slot):
            guarded(condition, copy.wait_send)

    def wait_recvs(slot):
        for came, (_, copy) in zip((below, above, None, below, above), copies(slot)):
            guarded(came, copy.wait_recv)

    def frame_copy(t, slot):
        return pltpu.make_async_copy(frames.at[jnp.minimum(t, steps - 1)], fr.at[slot], fr_sem.at[slot])

    weight_copies = []
    for k in range(3):
        taps = pl.ds(3 * k, 3)
        weight_copies.append([
            pltpu.make_async_copy(w_rec.at[taps, pl.ds(0, 128)], wraw.at[taps, pl.ds(0, 128)], in_sem.at[2 + 3 * k]),
            pltpu.make_async_copy(w_in.at[taps], wraw.at[taps, pl.ds(128, 64)], in_sem.at[3 + 3 * k]),
            pltpu.make_async_copy(w_rec.at[taps, pl.ds(128, 64)], wraw.at[taps, pl.ds(192, 64)], in_sem.at[4 + 3 * k]),
        ])
    state_copies = [pltpu.make_async_copy(h_hbm, hb, in_sem.at[0]), pltpu.make_async_copy(c_hbm, cb, in_sem.at[1])]

    bias = lane_order(gate_bias[...].reshape(1, 768), 192)
    lane = lax.broadcasted_iota(jnp.int32, (tw, 128), 1)
    low = lane < 64
    scale = jnp.where(low, 1.0, 0.5)
    shift = jnp.where(low, 0.0, 0.5)
    x = (xm, xt)
    inner = (1 - col) * (tw - 1)
    edges = (em, et)
    own, beside, beyond = 1, 2 * col, 2 - 2 * col

    def base(i):
        return PAD + (i + 1) * PITCH + 8

    def row_at(i):
        return pl.ds(base(i), tw)

    def col_at(j, first=0, size=th):
        return pl.ds(base(first) + j, size, stride=PITCH)

    def dot(lhs):
        return lax.dot_general(jnp.concatenate(lhs, axis=1), ws[...], (((1,), (0,)), ((), ())), preferred_element_type=F32)

    def row_parts(rows, dy, dx):
        return [jnp.concatenate([part[pl.ds(base(i + dy - 1) + dx - 1, tw), :] for i in rows], axis=0) for part in x]

    def matmul(g_ref, block):
        rows = range(block[0], sum(block))
        g_ref[...] = dot([v for dy in range(3) for dx in range(3) for v in row_parts(rows, dy, dx)])

    def ring_matmul():
        lhs = []
        for dy in range(3):
            for dx in range(3):
                for part, value in enumerate(row_parts(RING_ROWS, dy, dx)):
                    lhs.append(jnp.concatenate([value, edges[part][dx, pl.ds(PAD - 1 + dy, th), :]], axis=0))
        gr[...] = dot(lhs)

    def cell(gates, c_main, c_tail, frame):
        pre = [gates(k) + bias[:, 128 * k:128 * (k + 1)] for k in range(6)]
        n_main = half_tanh(pre[1]) * c_main + half_tanh(pre[0]) * jnp.tanh(pre[3])
        h_main = half_tanh(pre[2]) * jnp.tanh(n_main)
        fore = half_tanh(pre[4])
        back = jnp.tanh(pre[5] * scale) * scale + shift
        n_tail = fore * c_tail + pltpu.roll(fore * back, 64, 1)
        return n_main, n_tail, h_main, jnp.where(low, frame, back * jnp.tanh(n_tail))

    def update_row(g_ref, g_row, i):
        at = pl.ds(i * tw, tw)
        cm[at, :], ct[at, :], xm[row_at(i), :], xt[row_at(i), :] = cell(
            lambda k: g_ref[pl.ds(g_row, tw), 128 * k:128 * (k + 1)], cm[at, :], ct[at, :], fx[at, :])

    def update_rows(g_ref, block, rows):
        for i in rows:
            update_row(g_ref, (i - block[0]) * tw, i)

    def update_ring():
        update_row(gr, 0, 0)
        update_row(gr, 2 * tw, th - 1)
        g_row = len(RING_ROWS) * tw
        colm[...], colt[...], *values = cell(
            lambda k: gr[pl.ds(g_row, th), 128 * k:128 * (k + 1)], colm[...], colt[...], fx[pl.ds(inner, th, stride=tw), :])
        for part, value in enumerate(values):
            edges[part][own, PAD:PAD + th, :] = value
            x[part][col_at(inner, 0, th - 8), :] = value[:th - 8]
            x[part][pl.ds(base(th - 1) + inner, 1), :] = value[th - 1:]
            send[SIDE, :, 128 * part:128 * (part + 1)] = value.astype(BF16)
        fill_row_sends()

    def fill_row_sends():
        for place, i in ((UP, 0), (DOWN, th - 1)):
            for part in range(2):
                send[place, :, 128 * part:128 * (part + 1)] = x[part][row_at(i), :].astype(BF16)

    def keep_beside():
        for part, e in enumerate(edges):
            e[beside, PAD:PAD + th, :] = x[part][col_at(inner + 1 - beyond), :]

    def finish_step():
        update_rows(gc, BLOCK_C, [sum(BLOCK_C) - 1])
        update_rows(gd, BLOCK_D, range(BLOCK_D[0], sum(BLOCK_D)))
        update_row(gr, tw, 30)
        for part, e in enumerate(edges):
            x[part][col_at(inner, th - 8, 8), :] = e[own, PAD + th - 8:PAD + th, :]
        keep_beside()

    def form_out(t):
        for i in range(th):
            at = pl.ds(i * tw, tw)
            hs[t, at, 0:128] = x[0][row_at(i), :].astype(BF16)
            hs[t, at, 128:192] = pltpu.roll(x[1][row_at(i), :], 64, 1)[:, :64].astype(BF16)

    def convert_frame(slot):
        for i in range(th):
            at = pl.ds(i * tw, tw)
            fx[at, 0:64] = fr[slot, at, :].astype(F32)

    def place_halo(slot):
        for part, e in enumerate(edges):
            lanes = slice(128 * part, 128 * (part + 1))
            for place, i in ((UP, -1), (DOWN, th)):
                x[part][row_at(i), :] = land[slot, place, :, lanes].astype(F32)
                value = corner[slot, place, :, lanes].astype(F32)
                value = jnp.where(col == 0, value[0:1, :], value[half - 1:, :])
                x[part][pl.ds(base(i) + inner + 1 - 2 * col, 1), :] = value
            e[beyond, PAD:PAD + th, :] = land[slot, SIDE, :, lanes].astype(F32)
            for k in range(3):
                for i in (-1, th):
                    e[k, PAD + i:PAD + i + 1, :] = x[part][pl.ds(base(i) + inner - 1 + k, 1), :]

    def late_blocks():
        ring_matmul()
        update_rows(ga, BLOCK_A, [1])
        update_rows(gb, BLOCK_B, [sum(BLOCK_B) - 1])
        update_rows(gc, BLOCK_C, range(BLOCK_C[0], sum(BLOCK_C) - 1))
        matmul(gd, BLOCK_D)
        update_ring()

    def early_blocks(t, frame_slot):
        matmul(ga, BLOCK_A)
        if t is not None:
            finish_step()
            form_out(t)
        convert_frame(frame_slot)
        matmul(gb, BLOCK_B)
        update_rows(ga, BLOCK_A, range(2, sum(BLOCK_A) - 1))
        matmul(gc, BLOCK_C)
        update_rows(ga, BLOCK_A, [sum(BLOCK_A) - 1])
        update_rows(gb, BLOCK_B, range(BLOCK_B[0], sum(BLOCK_B) - 1))

    for copy in sum(weight_copies, []):
        copy.start()
    frame_copy(0, 0).start()
    for copy in state_copies:
        copy.start()
    frame_copy(1, 1).start()
    land[...] = jnp.zeros_like(land)
    corner[...] = jnp.zeros_like(corner)
    barrier = pltpu.get_barrier_semaphore()
    neighbours = 1 + 2 * above.astype(jnp.int32) + 2 * below.astype(jnp.int32)
    for condition, d_row, d_col, *_ in routes(0):
        guarded(condition, functools.partial(
            pl.semaphore_signal, barrier, inc=1, device_id={"rows": row + d_row, "cols": col + d_col}, device_id_type=MESH))
    for ref in (em, et, xm, xt):
        ref[...] = jnp.zeros_like(ref)
    fx[...] = jnp.zeros_like(fx)

    for k, chunk in enumerate(weight_copies):
        for copy in chunk:
            copy.wait()

        @pl.loop(3 * k, 3 * k + 3)
        def _(tap):
            for first in range(0, 256, 64):
                at = pl.ds(pl.multiple_of(tap * 256 + first, 64), 64)
                ws[at, :] = lane_order(wraw[tap, first:first + 64, :], 192)
    frame_copy(0, 0).wait()
    for copy in state_copies:
        copy.wait()

    @pl.loop(0, th, step=8)
    def _(first):
        for k in range(8):
            i = first + k
            at = pl.ds(pl.multiple_of(i * tw, tw), tw)
            to = pl.ds(pl.multiple_of(base(0) + i * PITCH, 8), tw)
            xm[to, :] = hb[at, 0:128].astype(F32)
            tail = hb[at, 128:192].astype(F32)
            xt[to, :] = jnp.concatenate([fr[0, at, :].astype(F32), tail], axis=1)
            cm[at, :] = cb[at, 0:128]
            tail = cb[at, 128:192]
            ct[at, :] = jnp.concatenate([tail, tail], axis=1)

    colm[...] = cm[pl.ds(inner, th, stride=tw), :]
    colt[...] = ct[pl.ds(inner, th, stride=tw), :]
    for part in range(2):
        value = x[part][col_at(inner), :]
        edges[part][own, PAD:PAD + th, :] = value
        send[SIDE, :, 128 * part:128 * (part + 1)] = value.astype(BF16)
    keep_beside()
    fill_row_sends()
    pl.semaphore_wait(barrier, neighbours)
    start_sends(0)
    frame_copy(1, 1).wait()
    frame_copy(2, 0).start()
    early_blocks(None, 1)

    def arrive(slot):
        wait_recvs(slot)
        wait_sends(slot)
        place_halo(slot)

    def body(t, carry):
        slot = lax.rem(t, 2)
        frame_copy(t + 2, slot).wait()
        frame_copy(t + 3, 1 - slot).start()
        arrive(slot)
        late_blocks()
        start_sends(1 - slot)
        early_blocks(t, slot)
        return carry

    last = steps - 1
    lax.fori_loop(0, last, body, 0)
    frame_copy(last + 2, last % 2).wait()
    arrive(last % 2)
    late_blocks()
    finish_step()
    form_out(last)
    cm[pl.ds(inner, th, stride=tw), :] = colm[...]
    ct[pl.ds(inner, th, stride=tw), :] = colt[...]

    for i in range(th):
        at = pl.ds(i * tw, tw)
        c_out[at, 0:128] = cm[at, :]
        c_out[at, 128:192] = pltpu.roll(ct[at, :], 64, 1)[:, :64]


def write_kernel(hs, c, hs_hbm, c_hbm, sems):
    copies = [pltpu.make_async_copy(hs.at[t], hs_hbm.at[t], sems.at[t]) for t in range(hs.shape[0])]
    copies.append(pltpu.make_async_copy(c, c_hbm, sems.at[hs.shape[0]]))
    for k, copy in enumerate(copies):
        copy.start(priority=k % 2)
    for copy in copies:
        copy.wait()


def lane_order(x, c):
    i, f, o, g = (x[..., k * c:(k + 1) * c] for k in range(4))
    return jnp.concatenate([i[..., :128], f[..., :128], o[..., :128], g[..., :128],
                            i[..., 128:], f[..., 128:], g[..., 128:], o[..., 128:]], axis=-1)


def solution(mesh):
    n_rows, n_cols = mesh.shape["rows"], mesh.shape["cols"]
    seq_spec = P(None, "dp", "rows", "cols", None)
    state_spec = P("dp", "rows", "cols", None)

    def local_run(frames, w_in, w_rec, gate_bias, h_init, c_init):
        steps, _, th, tw, c_in = frames.shape
        c_hid = h_init.shape[-1]
        cells = th * tw
        vmem = pl.BlockSpec(memory_space=pltpu.VMEM)
        hbm = pl.BlockSpec(memory_space=pl.ANY)
        run = pl.pallas_call(
            functools.partial(kernel, n_rows, n_cols, steps, th, tw),
            out_shape=(pltpu.VMEM((steps, cells, c_hid), BF16), pltpu.VMEM((cells, c_hid), F32)),
            in_specs=[hbm, hbm, hbm, vmem, hbm, hbm],
            out_specs=(vmem, vmem),
            scratch_shapes=[
                *[pltpu.VMEM((PAD + (th + 2) * PITCH + PAD, 128), F32)] * 2,
                pltpu.VMEM((cells, 128), F32),
                *[pltpu.VMEM((3, th + 2 * PAD, 128), F32)] * 2,
                *[pltpu.VMEM((cells, 128), F32)] * 2,
                *[pltpu.VMEM((th, 128), F32)] * 2,
                *[pltpu.VMEM((block[1] * tw, 768), F32) for block in (BLOCK_A, BLOCK_B, BLOCK_C, BLOCK_D)],
                pltpu.VMEM(((len(RING_ROWS) + 1) * tw, 768), F32),
                pltpu.VMEM((9, c_in + c_hid, 4 * c_hid), BF16),
                pltpu.VMEM((9 * (c_in + c_hid), 4 * c_hid), BF16),
                pltpu.VMEM((cells, c_hid), BF16),
                pltpu.VMEM((cells, c_hid), F32),
                pltpu.VMEM((2, cells, c_in), BF16),
                pltpu.VMEM((3, tw, 256), BF16),
                pltpu.VMEM((2, 3, tw, 256), BF16),
                pltpu.VMEM((2, 2, tw // 2, 256), BF16),
                pltpu.SemaphoreType.DMA((5,)),
                pltpu.SemaphoreType.DMA((2, 5)),
                pltpu.SemaphoreType.DMA((2,)),
                pltpu.SemaphoreType.DMA((11,)),
            ],
            compiler_params=pltpu.CompilerParams(collective_id=0, has_side_effects=True, vmem_limit_bytes=40 << 20),
        )
        hidden, c_last = run(frames.reshape(steps, cells, c_in), w_in.reshape(9, c_in, -1), w_rec.reshape(9, c_hid, -1),
                             gate_bias, h_init.reshape(cells, c_hid), c_init.reshape(cells, c_hid))
        hidden, c_last = pl.pallas_call(
            write_kernel,
            out_shape=(jax.ShapeDtypeStruct(hidden.shape, BF16), jax.ShapeDtypeStruct(c_last.shape, F32)),
            in_specs=[vmem, vmem],
            out_specs=(hbm, hbm),
            scratch_shapes=[pltpu.SemaphoreType.DMA((steps + 1,))],
            compiler_params=pltpu.CompilerParams(vmem_limit_bytes=1 << 20),
        )(hidden, c_last)
        return hidden.reshape(steps, 1, th, tw, c_hid), c_last.reshape(1, th, tw, c_hid)

    return jax.shard_map(local_run, mesh=mesh, in_specs=(seq_spec, P(), P(), P(), state_spec, state_spec),
                         out_specs=(seq_spec, state_spec), check_vma=False)
```
